256 devices in a mesh: row: 16 (over z, x_lo), col: 16 (over y, x_hi, core).
Axes of the slice: x: 4 (x_hi: 2, x_lo: 2; x = x_hi * 2 + x_lo), y: 4, z: 8, core: 2. Of those that a mesh axis runs over, the one named last changes fastest.
Arguments:
- matrix: float32 [512, 32, 128, 128], P('row', 'col'), may hold values from -0.09375 to 0.09375
- columns: int32 [512, 32], P('row', 'col'), may hold values from 0 to 31
- counts: int32 [512, 16], P('row', 'col'), may hold values from 1 to 2
- fine_guess: float32 [512, 32, 128], P(('col', 'row')), may hold values from -6 to 6
- right_side: float32 [512, 32, 128], P(('row', 'col')), may hold values from -6 to 6
- aggregate: int32 [512], P(('row', 'col')), may hold values from 0 to 7
- restrict: float32 [512, 128, 128], P(('row', 'col')), may hold values from -0.5 to 0.5
Outputs:
- coarse_scaled: float32 [128, 32, 128], P('row')
- residual: float32 [512, 32, 128], P(('row', 'col'))
The draws below stay inside these ranges and needn't reach their ends.
Inputs may be any that keep to these rules, and one draw needn't show every extreme that they name: `counts`: slots at or past the count hold no part of the operator.
All inputs are finite; a program needn't handle non-finite values.
Results may differ from the reference program's by a relative error of at most 0.000071.
Values sent between devices are 32-bit elements; how exact they have to be, the bound alone decides.
A program may use at most 64 MiB of HBM per device.

```python
import jax
import jax.numpy as jnp
from jax import lax

BS = 128
CW = 128
KB = 2
NC_GRP = 8
BR_DEV = 2
NV = 32
GR = 32
CG = 32
NB = 512
N_ROW = 16
N_COL = 16


def place_ends(values, own_key, low, high):
    dims = values.shape
    index_at = [jax.random.randint(jax.random.fold_in(own_key, axis), (), 0, dims[axis]) for axis in range(len(dims))]
    values = values.at[tuple(index_at)].set(low)
    longest = dims.index(max(dims))
    index_at[longest] = (index_at[longest] + 1) % dims[longest]
    return values.at[tuple(index_at)].set(high)


def block_levels(key, shape, shards, low, top_value):
    def one(dim, parts):
        draws = jax.random.uniform(jax.random.fold_in(jax.random.fold_in(key, 6), dim), (parts,), jnp.float32, low / len(shards), top_value / len(shards))
        return jnp.repeat(jnp.exp(draws), shape[dim] // parts).reshape((-1,) + (1,) * (len(shape) - dim - 1))

    factor_of = one(*shards[0])
    for cut in shards[1:]:
        factor_of = factor_of * one(*cut)
    return factor_of


def centred(rng, extent, width, limit, split=(), kind=jnp.bfloat16):
    array = jax.random.normal(rng, extent, jnp.float32) * width
    if len(split) > 0:
        array = block_levels(rng, extent, split, -0.22, 0.18) * array
    return jnp.clip(array, min=-limit, max=limit).astype(kind)


def setup_inputs(seed: int = 0) -> dict:
    keys = jax.random.split(jax.random.key(seed), 8)
    matrix = centred(keys[0], (NB, N_COL * KB, BS, BS), (BS * KB * N_COL) ** -0.5, 0.09375, ((0, 16), (1, 16)), jnp.float32)
    columns = place_ends(jax.random.randint(keys[1], (NB, N_COL * KB), 0, BR_DEV * N_ROW), jax.random.fold_in(keys[1], 1), 0, (BR_DEV * N_ROW) - 1).astype(jnp.int32)
    counts = place_ends(jax.random.randint(keys[2], (NB, N_COL), 1, KB + 1), jax.random.fold_in(keys[2], 1), 1, KB).astype(jnp.int32)
    fine_guess = centred(keys[3], (NB, NV, BS), 1.0, 6.0, ((0, 256),), jnp.float32)
    right_side = centred(keys[4], (NB, NV, BS), 1.0, 6.0, ((0, 256),), jnp.float32)
    aggregate = place_ends(jax.random.randint(keys[5], (NB,), 0, NC_GRP), jax.random.fold_in(keys[5], 1), 0, NC_GRP - 1).astype(jnp.int32)
    restrict = centred(keys[6], (NB, BS, CW), BS ** -0.5, 0.5, ((0, 256),), jnp.float32)
    return dict(matrix=matrix, columns=columns, counts=counts, fine_guess=fine_guess, right_side=right_side, aggregate=aggregate, restrict=restrict)


def reference(matrix, columns, counts, fine_guess, right_side, aggregate, restrict):
    slot_total = N_COL * KB
    slot_index = jnp.arange(slot_total, dtype=jnp.int32)
    slot_group = slot_index // KB
    global_col = (slot_group[None, :] * CG + columns).astype(jnp.int32)
    usable = (slot_index % KB)[None, :] < counts[:, slot_group]
    picked = fine_guess[global_col] * usable[:, :, None, None].astype(jnp.float32)
    product = jnp.einsum('gsab,gsvb->gva', matrix, picked, precision=lax.Precision.HIGHEST)
    residual = right_side - product
    mean_sq = lax.optimization_barrier(jnp.mean(residual * residual, axis=(0, 2)))
    scale_rms = jnp.sqrt(mean_sq + 1e-06)
    contrib = jnp.einsum('gva,gak->gvk', residual, restrict, precision=lax.Precision.HIGHEST)
    target = (jnp.arange(NB, dtype=jnp.int32) // GR * NC_GRP + aggregate).astype(jnp.int32)
    coarse = jax.ops.segment_sum(contrib, target, num_segments=NC_GRP * N_ROW)
    return (coarse / scale_rms[None, :, None], residual)
```

```python
import jax
import jax.numpy as jnp
from jax import lax
from jax.experimental import pallas as pl
from jax.experimental.pallas import tpu as pltpu
from jax.sharding import PartitionSpec as P

MESH = pl.DeviceIdType.MESH
F32 = jnp.float32
BF16 = jnp.bfloat16

NR, NC = 16, 16
NZ = NR // 2
NQ = NC // 2
GR, KB, NV, BS = 32, 2, 32, 128
NAGG = 8
CHUNKS = 4
Z_ORDER = (4, 3, 5, 2, 6, 1, 7)
Q_ORDER = ((2, 1), (1, 1), (3, 1), (2, 0), (0, 1), (1, 0), (3, 0), (0, 0))


def split(x):
    hi = x.astype(BF16)
    return hi, (x - hi.astype(F32)).astype(BF16)


def kernel(
    mat, cols, cnts, xin, rhs, agg, rest, coarse_out, resid_out,
    mraw, mw, xg, pout, pin, sb, rb, aout, ain, cbuf, sqb, rhs_v, rest_v, tmp, ov,
    cols_s, cnts_s, agg_s,
    mat_sem, loc_sem, ag_send, ag_recv, p_send, p_recv, s_send, s_recv,
    a_send, a_recv, b_send, b_recv, q_send, q_recv, out_sem,
):
    r = lax.axis_index("row")
    c = lax.axis_index("col")
    z, xl = r // 2, r % 2
    core, chip = c % 2, c // 2
    y, xh = chip // 2, chip % 2

    def remote(src, dst, ss, rs, row, col):
        return pltpu.make_async_remote_copy(
            src_ref=src, dst_ref=dst, send_sem=ss, recv_sem=rs,
            device_id=(row, col), device_id_type=MESH,
        )

    own_x = pltpu.make_async_copy(xin, xg.at[pl.ds(2 * r, 2)], loc_sem.at[0])
    own_x.start()
    per = GR // CHUNKS
    mats = [
        pltpu.make_async_copy(mat.at[pl.ds(k * per, per)], mraw.at[pl.ds(k * per, per)], mat_sem.at[k])
        for k in range(CHUNKS)
    ]
    for m in mats:
        m.start()
    smalls = [
        pltpu.make_async_copy(cols, cols_s, loc_sem.at[1]),
        pltpu.make_async_copy(cnts, cnts_s, loc_sem.at[2]),
        pltpu.make_async_copy(agg, agg_s, loc_sem.at[3]),
        pltpu.make_async_copy(rhs, rhs_v, loc_sem.at[4]),
        pltpu.make_async_copy(rest, rest_v, loc_sem.at[5]),
    ]
    for m in smalls:
        m.start()

    barrier = pltpu.get_barrier_semaphore()

    def greet(d, carry):
        pl.semaphore_signal(barrier, inc=1, device_id=((r + d) % NR, c), device_id_type=MESH)
        pl.semaphore_signal(barrier, inc=1, device_id=(r, (c + d) % NC), device_id_type=MESH)
        return carry

    lax.fori_loop(1, 16, greet, 0)
    own_x.wait()
    pl.semaphore_wait(barrier, NR - 1 + NC - 1)

    other = z * 2 + 1 - xl

    def ag(block_row, to_row, s):
        ref = xg.at[pl.ds(2 * block_row, 2)]
        return remote(ref, ref, ag_send.at[s], ag_recv.at[block_row], to_row, c)

    sends = []
    for i, d in enumerate(Z_ORDER):
        cp = ag(r, ((z + d) % NZ) * 2 + xl, i)
        cp.start()
        sends.append(cp)
    cp = ag(r, other, 7)
    cp.start()
    sends.append(cp)

    for k in range(CHUNKS):
        mats[k].wait()

        def parts(g, carry):
            for s in range(KB):
                hi, lo = split(mraw[g, s])
                mw[g, 0:BS, s * BS:(s + 1) * BS] = hi
                mw[g, BS:2 * BS, s * BS:(s + 1) * BS] = lo
            return carry

        lax.fori_loop(k * per, (k + 1) * per, parts, 0)

    for i, d in enumerate(Z_ORDER):
        zr = ((z + NZ - d) % NZ) * 2 + xl
        ag(zr, r, 0).wait_recv()
        cp = ag(zr, other, 8 + i)
        cp.start()
        sends.append(cp)
    for m in smalls:
        m.wait()
    for d in (0,) + Z_ORDER:
        ag(((z + NZ - d) % NZ) * 2 + 1 - xl, r, 0).wait_recv()

    def product(g):
        used = jnp.where(cnts_s[g, 0] > 1, 1.0, 0.0).astype(F32)
        x = jnp.concatenate([xg[cols_s[g, 0]], xg[cols_s[g, 1]] * used], axis=1)
        hi, lo = split(x)
        o = lax.dot_general(
            jnp.concatenate([hi, lo], axis=0), mw[g], (((1,), (1,)), ((), ())),
            preferred_element_type=F32,
        )
        return o[:NV, :BS] + (o[:NV, BS:] + o[NV:, :BS])

    def chip_of(d):
        return ((y + d[0]) % 4) * 2 + (xh + d[1]) % 2

    pair = chip * 2 + 1 - core
    for i, d in enumerate(Q_ORDER):
        q = chip_of(d)
        for k in range(2):
            pout[q, k] = product(4 * q + 2 * (1 - core) + k)
        cp = remote(pout.at[q], pin.at[q], p_send.at[i], p_recv.at[q], r, pair)
        cp.start()
        sends.append(cp)
    for i, d in enumerate(Q_ORDER):
        q = chip_of(d)
        for k in range(2):
            sb[q, k] = product(4 * q + 2 * core + k)
        remote(pout.at[q], pin.at[q], p_send.at[i], p_recv.at[q], r, pair).wait_recv()
        for k in range(2):
            sb[q, k] = sb[q, k] + pin[q, k]
        if d != (0, 0):
            cp = remote(sb.at[q], rb.at[chip], s_send.at[i], s_recv.at[chip], r, q * 2 + core)
            cp.start()
            sends.append(cp)

    total = [sb[chip, 0], sb[chip, 1]]
    for d in Q_ORDER[:-1]:
        q = chip_of(d)
        remote(sb.at[q], rb.at[q], s_send.at[0], s_recv.at[q], r, c).wait_recv()
        for k in range(2):
            total[k] = total[k] + rb[q, k]
    contrib = []
    sq = jnp.zeros((NV, BS), F32)
    for k in range(2):
        res = rhs_v[k] - total[k]
        tmp[k] = res
        sq = sq + res * res
        hi, lo = split(res)
        whi, wlo = split(rest_v[k])
        o = lax.dot_general(
            jnp.concatenate([hi, lo], axis=0), jnp.concatenate([whi, wlo], axis=1),
            (((1,), (0,)), ((), ())), preferred_element_type=F32,
        )
        tmp[2 + k] = o[:NV, :BS] + (o[:NV, BS:] + o[NV:, :BS])
    resid_cp = pltpu.make_async_copy(tmp.at[pl.ds(0, 2)], resid_out, out_sem.at[0])
    resid_cp.start()

    lane = lax.broadcasted_iota(jnp.int32, (NV, BS), 1)
    sub = lax.broadcasted_iota(jnp.int32, (NV, BS), 0)
    eye = lane == sub
    sq_row = jnp.sum(jnp.where(eye, jnp.sum(sq, axis=1, keepdims=True), 0.0), axis=0, keepdims=True)
    for k in range(2):
        for v in range(2):
            aout[pl.ds(2 * k + v, NC, stride=8), :] = tmp[2 + k, pl.ds(v, NC, stride=2), :]
        aout[pl.ds(5 + k, NC, stride=8), :] = jnp.full((NC, BS), agg_s[k].astype(F32), F32)
    aout[pl.ds(4, NC, stride=8), :] = jnp.broadcast_to(sq_row, (NC, BS))
    aout[pl.ds(7, NC, stride=8), :] = jnp.zeros((NC, BS), F32)

    def tile(ref, j):
        return ref.at[pl.ds(pl.multiple_of(8 * j, 8), 8)]

    for d in range(1, NC):
        j = (c + d) % NC
        cp = remote(tile(aout, j), tile(ain, c), a_send.at[d], a_recv.at[c], r, j)
        cp.start()
        sends.append(cp)
    tile(ain, c)[...] = tile(aout, c)[...]

    who = lax.broadcasted_iota(jnp.int32, (NAGG, BS), 0).astype(F32)
    acc = [jnp.zeros((NAGG, BS), F32) for _ in range(2)]
    group_sq = jnp.zeros((1, BS), F32)
    for d in range(NC):
        j = (c + NC - d) % NC
        if d > 0:
            remote(tile(aout, j), tile(ain, j), a_send.at[0], a_recv.at[j], r, c).wait_recv()
        t = tile(ain, j)[...]
        for k in range(2):
            sel = who == t[5 + k:6 + k, :]
            for v in range(2):
                acc[v] = acc[v] + jnp.where(sel, t[2 * k + v:2 * k + v + 1, :], 0.0)
        group_sq = group_sq + t[4:5, :]
    tile(sqb, r)[...] = jnp.broadcast_to(group_sq, (8, BS))
    for d in range(1, NR):
        j = (r + d) % NR
        cp = remote(tile(sqb, r), tile(sqb, r), q_send.at[d], q_recv.at[r], j, c)
        cp.start()
        sends.append(cp)

    def slot(j):
        return cbuf.at[pl.ds(pl.multiple_of(16 * j, 16), 16)]

    slot(c)[0:8, :] = acc[0]
    slot(c)[8:16, :] = acc[1]
    for d in range(1, NC):
        j = (c + d) % NC
        cp = remote(slot(c), slot(c), b_send.at[d], b_recv.at[c], r, j)
        cp.start()
        sends.append(cp)

    all_sq = group_sq
    for d in range(1, NR):
        j = (r + NR - d) % NR
        remote(tile(sqb, j), tile(sqb, j), q_send.at[0], q_recv.at[j], r, c).wait_recv()
        all_sq = all_sq + tile(sqb, j)[0:1, :]
    mean = all_sq * (1.0 / (NR * GR * BS)) + 1e-6
    mean_v = jnp.sum(jnp.where(eye, jnp.broadcast_to(mean, (NV, BS)), 0.0), axis=1, keepdims=True)
    inv = jnp.broadcast_to(1.0 / jnp.sqrt(mean_v), (NV, BS))
    for d in range(1, NC):
        j = (c + NC - d) % NC
        remote(slot(j), slot(j), b_send.at[0], b_recv.at[j], r, c).wait_recv()
    for a in range(NAGG):
        ov[a] = cbuf[pl.ds(a, NV, stride=8), :] * inv
    coarse_out_cp = [
        pltpu.make_async_copy(ov, coarse_out, out_sem.at[1])
    ]
    for cp in sends:
        cp.wait_send()
    for cp in coarse_out_cp:
        cp.start()
    for cp in coarse_out_cp:
        cp.wait()
    resid_cp.wait()


def local(matrix, columns, counts, fine_guess, right_side, aggregate, restrict):
    dma = pltpu.SemaphoreType.DMA
    return pl.pallas_call(
        kernel,
        out_shape=(
            jax.ShapeDtypeStruct((NAGG, NV, BS), F32),
            jax.ShapeDtypeStruct((2, NV, BS), F32),
        ),
        in_specs=[pl.BlockSpec(memory_space=pl.ANY)] * 7,
        out_specs=(pl.BlockSpec(memory_space=pl.ANY),) * 2,
        scratch_shapes=[
            pltpu.VMEM((GR, KB, BS, BS), F32),
            pltpu.VMEM((GR, 2 * BS, KB * BS), BF16),
            pltpu.VMEM((2 * NR, NV, BS), F32),
            pltpu.VMEM((NQ, 2, NV, BS), F32),
            pltpu.VMEM((NQ, 2, NV, BS), F32),
            pltpu.VMEM((NQ, 2, NV, BS), F32),
            pltpu.VMEM((NQ, 2, NV, BS), F32),
            pltpu.VMEM((NC * 8, BS), F32),
            pltpu.VMEM((NC * 8, BS), F32),
            pltpu.VMEM((NC * 16, BS), F32),
            pltpu.VMEM((NR * 8, BS), F32),
            pltpu.VMEM((2, NV, BS), F32),
            pltpu.VMEM((2, BS, BS), F32),
            pltpu.VMEM((4, NV, BS), F32),
            pltpu.VMEM((NAGG, NV, BS), F32),
            pltpu.SMEM((GR, KB), jnp.int32),
            pltpu.SMEM((GR, 1), jnp.int32),
            pltpu.SMEM((2,), jnp.int32),
            dma((CHUNKS,)), dma((6,)),
            dma((16,)), dma((NR,)),
            dma((NQ,)), dma((NQ,)),
            dma((NQ,)), dma((NQ,)),
            dma((NC,)), dma((NC,)),
            dma((NC,)), dma((NC,)),
            dma((NR,)), dma((NR,)),
            dma((2,)),
        ],
        compiler_params=pltpu.CompilerParams(collective_id=0, has_side_effects=True),
    )(matrix, columns, counts, fine_guess, right_side, aggregate, restrict)


def solution(mesh):
    in_specs = (
        P("row", "col", None, None),
        P("row", "col"),
        P("row", "col"),
        P(("col", "row"), None, None),
        P(("row", "col"), None, None),
        P(("row", "col")),
        P(("row", "col"), None, None),
    )
    out_specs = (P("row", None, None), P(("row", "col"), None, None))
    return jax.shard_map(local, mesh=mesh, in_specs=in_specs, out_specs=out_specs, check_vma=False)
```

```python
import jax
import jax.numpy as jnp
from jax import lax
from jax.experimental import pallas as pl
from jax.experimental.pallas import tpu as pltpu
from jax.sharding import PartitionSpec as P

MESH = pl.DeviceIdType.MESH
F32 = jnp.float32
BF16 = jnp.bfloat16

NR, NC = 16, 16
NZ = NR // 2
NQ = NC // 2
GR, KB, NV, BS = 32, 2, 32, 128
NAGG = 8
CHUNKS = 4
Z_ORDER = (4, 3, 5, 2, 6, 1, 7)
Q_ORDER = ((2, 1), (1, 1), (3, 1), (2, 0), (0, 1), (1, 0), (3, 0), (0, 0))


def split(x):
    hi = x.astype(BF16)
    return hi, (x - hi.astype(F32)).astype(BF16)


def diagonal():
    lane = lax.broadcasted_iota(jnp.int32, (NV, BS), 1)
    return lane == lax.broadcasted_iota(jnp.int32, (NV, BS), 0)


def kernel(
    mat, cols, cnts, xin, rhs, agg, rest, cbuf, sqb, resid,
    mraw, mw, xg, pout, pin, sb, rb, aout, ain, rhs_v, rest_v, tmp,
    cols_s, cnts_s, agg_s,
    mat_sem, loc_sem, ag_send, ag_recv, p_send, p_recv, s_send, s_recv,
    a_send, a_recv, b_send, b_recv, q_send, q_recv,
):
    r = lax.axis_index("row")
    c = lax.axis_index("col")
    z, xl = r // 2, r % 2
    core, chip = c % 2, c // 2
    y, xh = chip // 2, chip % 2

    def remote(src, dst, ss, rs, row, col):
        return pltpu.make_async_remote_copy(
            src_ref=src, dst_ref=dst, send_sem=ss, recv_sem=rs,
            device_id=(row, col), device_id_type=MESH,
        )

    sends = []
    own_x = pltpu.make_async_copy(xin, xg.at[pl.ds(2 * r, 2)], loc_sem.at[0])
    own_x.start()
    per = GR // CHUNKS
    mats = [
        pltpu.make_async_copy(mat.at[pl.ds(k * per, per)], mraw.at[pl.ds(k * per, per)], mat_sem.at[k])
        for k in range(CHUNKS)
    ]
    for m in mats:
        m.start()
    smalls = [
        pltpu.make_async_copy(cols, cols_s, loc_sem.at[1]),
        pltpu.make_async_copy(cnts, cnts_s, loc_sem.at[2]),
        pltpu.make_async_copy(agg, agg_s, loc_sem.at[3]),
        pltpu.make_async_copy(rhs, rhs_v, loc_sem.at[4]),
        pltpu.make_async_copy(rest, rest_v, loc_sem.at[5]),
    ]
    for m in smalls:
        m.start()

    barrier = pltpu.get_barrier_semaphore()

    def greet(d, carry):
        pl.semaphore_signal(barrier, inc=1, device_id=((r + d) % NR, c), device_id_type=MESH)
        pl.semaphore_signal(barrier, inc=1, device_id=(r, (c + d) % NC), device_id_type=MESH)
        return carry

    lax.fori_loop(1, 16, greet, 0)
    own_x.wait()
    pl.semaphore_wait(barrier, NR - 1 + NC - 1)

    other = z * 2 + 1 - xl

    def ag(block_row, to_row, s):
        ref = xg.at[pl.ds(2 * block_row, 2)]
        return remote(ref, ref, ag_send.at[s], ag_recv.at[block_row], to_row, c)

    for i, d in enumerate(Z_ORDER):
        cp = ag(r, ((z + d) % NZ) * 2 + xl, i)
        cp.start()
        sends.append(cp)
    cp = ag(r, other, 7)
    cp.start()
    sends.append(cp)

    for k in range(CHUNKS):
        mats[k].wait()

        def parts(g, carry):
            for s in range(KB):
                hi, lo = split(mraw[g, s])
                mw[g, 0:BS, s * BS:(s + 1) * BS] = hi
                mw[g, BS:2 * BS, s * BS:(s + 1) * BS] = lo
            return carry

        lax.fori_loop(k * per, (k + 1) * per, parts, 0)

    for i, d in enumerate(Z_ORDER):
        zr = ((z + NZ - d) % NZ) * 2 + xl
        ag(zr, r, 0).wait_recv()
        cp = ag(zr, other, 8 + i)
        cp.start()
        sends.append(cp)
    for m in smalls:
        m.wait()
    for d in (0,) + Z_ORDER:
        ag(((z + NZ - d) % NZ) * 2 + 1 - xl, r, 0).wait_recv()

    def product(g):
        used = jnp.where(cnts_s[0, g] > 1, 1.0, 0.0).astype(F32)
        x = jnp.concatenate([xg[cols_s[0, g]], xg[cols_s[1, g]] * used], axis=1)
        hi, lo = split(x)
        o = lax.dot_general(
            jnp.concatenate([hi, lo], axis=0), mw[g], (((1,), (1,)), ((), ())),
            preferred_element_type=F32,
        )
        return o[:NV, :BS] + (o[:NV, BS:] + o[NV:, :BS])

    def chip_of(d):
        return ((y + d[0]) % 4) * 2 + (xh + d[1]) % 2

    pair = chip * 2 + 1 - core
    for i, d in enumerate(Q_ORDER):
        q = chip_of(d)
        for k in range(2):
            pout[q, k] = product(4 * q + 2 * (1 - core) + k)
        cp = remote(pout.at[q], pin.at[q], p_send.at[i], p_recv.at[q], r, pair)
        cp.start()
        sends.append(cp)
    for i, d in enumerate(Q_ORDER):
        q = chip_of(d)
        for k in range(2):
            sb[q, k] = product(4 * q + 2 * core + k)
        remote(pout.at[q], pin.at[q], p_send.at[i], p_recv.at[q], r, pair).wait_recv()
        for k in range(2):
            sb[q, k] = sb[q, k] + pin[q, k]
        if d != (0, 0):
            cp = remote(sb.at[q], rb.at[chip], s_send.at[i], s_recv.at[chip], r, q * 2 + core)
            cp.start()
            sends.append(cp)

    total = [sb[chip, 0], sb[chip, 1]]
    for d in Q_ORDER[:-1]:
        q = chip_of(d)
        remote(sb.at[q], rb.at[q], s_send.at[0], s_recv.at[q], r, c).wait_recv()
        for k in range(2):
            total[k] = total[k] + rb[q, k]
    contrib = []
    sq = jnp.zeros((NV, BS), F32)
    for k in range(2):
        res = rhs_v[k] - total[k]
        resid[k] = res
        sq = sq + res * res
        hi, lo = split(res)
        whi, wlo = split(rest_v[k])
        o = lax.dot_general(
            jnp.concatenate([hi, lo], axis=0), jnp.concatenate([whi, wlo], axis=1),
            (((1,), (0,)), ((), ())), preferred_element_type=F32,
        )
        tmp[k] = o[:NV, :BS] + (o[:NV, BS:] + o[NV:, :BS])

    eye = diagonal()
    sq_row = jnp.sum(jnp.where(eye, jnp.sum(sq, axis=1, keepdims=True), 0.0), axis=0, keepdims=True)
    for k in range(2):
        for v in range(2):
            aout[pl.ds(2 * k + v, NC, stride=8), :] = tmp[k, pl.ds(v, NC, stride=2), :]
        aout[pl.ds(5 + k, NC, stride=8), :] = jnp.full((NC, BS), agg_s[k].astype(F32), F32)
    aout[pl.ds(4, NC, stride=8), :] = jnp.broadcast_to(sq_row, (NC, BS))
    aout[pl.ds(7, NC, stride=8), :] = jnp.zeros((NC, BS), F32)

    def tile(ref, j):
        return ref.at[pl.ds(pl.multiple_of(8 * j, 8), 8)]

    for d in range(1, NC):
        j = (c + d) % NC
        cp = remote(tile(aout, j), tile(ain, c), a_send.at[d], a_recv.at[c], r, j)
        cp.start()
        sends.append(cp)
    tile(ain, c)[...] = tile(aout, c)[...]

    who = lax.broadcasted_iota(jnp.int32, (NAGG, BS), 0).astype(F32)
    acc = [jnp.zeros((NAGG, BS), F32) for _ in range(2)]
    group_sq = jnp.zeros((1, BS), F32)
    for d in range(NC):
        j = (c + NC - d) % NC
        if d > 0:
            remote(tile(aout, j), tile(ain, j), a_send.at[0], a_recv.at[j], r, c).wait_recv()
        t = tile(ain, j)[...]
        for k in range(2):
            sel = who == t[5 + k:6 + k, :]
            for v in range(2):
                acc[v] = acc[v] + jnp.where(sel, t[2 * k + v:2 * k + v + 1, :], 0.0)
        group_sq = group_sq + t[4:5, :]
    tile(sqb, r)[...] = jnp.broadcast_to(group_sq, (8, BS))
    for d in range(1, NR):
        j = (r + d) % NR
        cp = remote(tile(sqb, r), tile(sqb, r), q_send.at[d], q_recv.at[r], j, c)
        cp.start()
        sends.append(cp)

    def slot(j):
        return cbuf.at[pl.ds(pl.multiple_of(16 * j, 16), 16)]

    slot(c)[0:8, :] = acc[0]
    slot(c)[8:16, :] = acc[1]
    for d in range(1, NC):
        j = (c + d) % NC
        cp = remote(slot(c), slot(c), b_send.at[d], b_recv.at[c], r, j)
        cp.start()
        sends.append(cp)

    for d in range(1, NR):
        j = (r + NR - d) % NR
        remote(tile(sqb, j), tile(sqb, j), q_send.at[0], q_recv.at[j], r, c).wait_recv()
    for d in range(1, NC):
        j = (c + NC - d) % NC
        remote(slot(j), slot(j), b_send.at[0], b_recv.at[j], r, c).wait_recv()
    for cp in sends:
        cp.wait_send()


def finish(cbuf, sqb, resid, coarse_out, resid_out):
    all_sq = jnp.sum(sqb[...], axis=0, keepdims=True) * 0.125
    mean = all_sq * (1.0 / (NR * GR * BS)) + 1e-6
    mean_v = jnp.sum(jnp.where(diagonal(), jnp.broadcast_to(mean, (NV, BS)), 0.0), axis=1, keepdims=True)
    inv = jnp.broadcast_to(1.0 / jnp.sqrt(mean_v), (NV, BS))
    for a in range(NAGG):
        coarse_out[a] = cbuf[pl.ds(a, NV, stride=8), :] * inv
    resid_out[...] = resid[...]


def local(matrix, columns, counts, fine_guess, right_side, aggregate, restrict):
    dma = pltpu.SemaphoreType.DMA
    vmem = pl.BlockSpec(memory_space=pltpu.VMEM)
    parts = pl.pallas_call(
        kernel,
        out_shape=(
            pltpu.VMEM((NC * 16, BS), F32),
            pltpu.VMEM((NR * 8, BS), F32),
            pltpu.VMEM((2, NV, BS), F32),
        ),
        in_specs=[pl.BlockSpec(memory_space=pltpu.HBM)] * 7,
        out_specs=(vmem,) * 3,
        scratch_shapes=[
            pltpu.VMEM((GR, KB, BS, BS), F32),
            pltpu.VMEM((GR, 2 * BS, KB * BS), BF16),
            pltpu.VMEM((2 * NR, NV, BS), F32),
            pltpu.VMEM((NQ, 2, NV, BS), F32),
            pltpu.VMEM((NQ, 2, NV, BS), F32),
            pltpu.VMEM((NQ, 2, NV, BS), F32),
            pltpu.VMEM((NQ, 2, NV, BS), F32),
            pltpu.VMEM((NC * 8, BS), F32),
            pltpu.VMEM((NC * 8, BS), F32),
            pltpu.VMEM((2, NV, BS), F32),
            pltpu.VMEM((2, BS, BS), F32),
            pltpu.VMEM((2, NV, BS), F32),
            pltpu.SMEM((KB, GR), jnp.int32),
            pltpu.SMEM((1, GR), jnp.int32),
            pltpu.SMEM((2,), jnp.int32),
            dma((CHUNKS,)), dma((6,)),
            dma((16,)), dma((NR,)),
            dma((NQ,)), dma((NQ,)),
            dma((NQ,)), dma((NQ,)),
            dma((NC,)), dma((NC,)),
            dma((NC,)), dma((NC,)),
            dma((NR,)), dma((NR,)),
        ],
        compiler_params=pltpu.CompilerParams(collective_id=0, has_side_effects=True, vmem_limit_bytes=60 * 2**20),
    )(matrix, columns.T, counts.T, fine_guess, right_side, aggregate, restrict)
    return pl.pallas_call(
        finish,
        out_shape=(
            jax.ShapeDtypeStruct((NAGG, NV, BS), F32),
            jax.ShapeDtypeStruct((2, NV, BS), F32),
        ),
        in_specs=[vmem] * 3,
        out_specs=(vmem,) * 2,
        compiler_params=pltpu.CompilerParams(vmem_limit_bytes=4 * 2**20),
    )(*parts)


def solution(mesh):
    in_specs = (
        P("row", "col", None, None),
        P("row", "col"),
        P("row", "col"),
        P(("col", "row"), None, None),
        P(("row", "col"), None, None),
        P(("row", "col")),
        P(("row", "col"), None, None),
    )
    out_specs = (P("row", None, None), P(("row", "col"), None, None))
    return jax.shard_map(local, mesh=mesh, in_specs=in_specs, out_specs=out_specs, check_vma=False)
```

```python
import jax
import jax.numpy as jnp
from jax import lax
from jax.experimental import pallas as pl
from jax.experimental.pallas import tpu as pltpu
from jax.sharding import PartitionSpec as P

MESH = pl.DeviceIdType.MESH
F32 = jnp.float32
BF16 = jnp.bfloat16

NR, NC = 16, 16
NZ = NR // 2
NQ = NC // 2
GR, KB, NV, BS = 32, 2, 32, 128
NAGG = 8
CHUNKS = 4
Q_ORDER = ((2, 1), (1, 1), (3, 1), (2, 0), (0, 1), (1, 0), (3, 0), (0, 0))


def split(x):
    hi = x.astype(BF16)
    return hi, (x - hi.astype(F32)).astype(BF16)


def diagonal():
    lane = lax.broadcasted_iota(jnp.int32, (NV, BS), 1)
    return lane == lax.broadcasted_iota(jnp.int32, (NV, BS), 0)


def kernel(
    mat, cols, cnts, xin, rhs, agg, rest, cbuf, sqb, resid,
    mraw, mw, xg, pout, pin, sb, rb, aout, ain, rhs_v, rest_v, rw, tmp, sqs, sqa,
    cols_s, cnts_s, agg_s,
    mat_sem, loc_sem, ag_send, ag_recv, p_send, p_recv, s_send, s_recv,
    a_send, a_recv, b_send, b_recv, o_send, o_recv, q_send, q_recv, tok,
):
    r = lax.axis_index("row")
    c = lax.axis_index("col")
    z, xl = r // 2, r % 2
    core, chip = c % 2, c // 2
    y, xh = chip // 2, chip % 2

    def remote(src, dst, ss, rs, row, col):
        return pltpu.make_async_remote_copy(
            src_ref=src, dst_ref=dst, send_sem=ss, recv_sem=rs,
            device_id=(row, col), device_id_type=MESH,
        )

    sends = []
    own_x = pltpu.make_async_copy(xin, xg.at[pl.ds(2 * r, 2)], loc_sem.at[0])
    own_x.start()
    per = GR // CHUNKS
    mats = [
        pltpu.make_async_copy(mat.at[pl.ds(k * per, per)], mraw.at[pl.ds(k * per, per)], mat_sem.at[k])
        for k in range(CHUNKS)
    ]
    for m in mats:
        m.start()
    smalls = [
        pltpu.make_async_copy(cols, cols_s, loc_sem.at[1]),
        pltpu.make_async_copy(cnts, cnts_s, loc_sem.at[2]),
        pltpu.make_async_copy(agg, agg_s, loc_sem.at[3]),
        pltpu.make_async_copy(rhs, rhs_v, loc_sem.at[4]),
        pltpu.make_async_copy(rest, rest_v, loc_sem.at[5]),
    ]
    for m in smalls:
        m.start()

    barrier = pltpu.get_barrier_semaphore()

    def z_row(d):
        return ((z + NZ + d) % NZ) * 2 + xl

    def chip_of(dy, dx):
        return ((y + dy) % 4) * 2 + (xh + dx) % 2

    def col_of(dy, dx):
        return chip_of(dy, dx) * 2 + core

    other = z * 2 + 1 - xl
    pair = chip * 2 + 1 - core
    near = [(z_row(d), c) for d in (2, -2, 1, -1)]
    near += [(other, c), (r, col_of(0, 1)), (r, col_of(1, 0)), (r, col_of(3, 0)), (r, pair)]
    for dev in near:
        pl.semaphore_signal(barrier, inc=1, device_id=dev, device_id_type=MESH)
    own_x.wait()
    pl.semaphore_wait(barrier, len(near))

    def ag(row, half, to_row):
        if half is None:
            ref, sem = xg.at[pl.ds(2 * row, 2)], 2 * row
        else:
            ref, sem = xg.at[pl.ds(2 * row + half, 1)], 2 * row + half
        return remote(ref, ref, ag_send.at[len(sends)], ag_recv.at[sem], to_row, c)

    def pass_on(row, half, *targets):
        for to_row in targets:
            cp = ag(row, half, to_row)
            cp.start()
            sends.append(cp)

    def arrived(row, half=None):
        ag(row, half, r).wait_recv()

    def across(d):
        return ((z + NZ + d) % NZ) * 2 + 1 - xl

    pass_on(r, None, other, z_row(2), z_row(-2), z_row(1), z_row(-1))
    for dy in (1, 3):
        pl.semaphore_signal(tok.at[0], inc=1, device_id=(r, col_of(dy, 0)), device_id_type=MESH)
    arrived(other)
    pass_on(other, None, z_row(1), z_row(-1))
    for s in (1, -1):
        arrived(z_row(-2 * s))
        pass_on(z_row(-2 * s), None, other, z_row(s))
        pass_on(z_row(-2 * s), (1 - s) // 2, z_row(2 * s))
    pl.semaphore_wait(tok.at[0], 2)
    pl.semaphore_signal(tok.at[1], inc=1, device_id=(r, col_of(0, 1)), device_id_type=MESH)
    for s in (1, -1):
        arrived(z_row(-3 * s))
        pass_on(z_row(-3 * s), None, other)
    for half in (0, 1):
        arrived(z_row(4), half)
        pass_on(z_row(4), half, other)

    for k in range(CHUNKS):
        mats[k].wait()

        def parts(g, carry):
            for s in range(KB):
                hi, lo = split(mraw[g, s])
                mw[g, 0:BS, s * BS:(s + 1) * BS] = hi
                mw[g, BS:2 * BS, s * BS:(s + 1) * BS] = lo
            return carry

        lax.fori_loop(k * per, (k + 1) * per, parts, 0)
    for m in smalls:
        m.wait()
    for k in range(2):
        whi, wlo = split(rest_v[k])
        rw[k, :, 0:BS] = whi
        rw[k, :, BS:2 * BS] = wlo
    for s in (1, -1):
        arrived(z_row(s))
        arrived(across(s))
        arrived(across(2 * s))
    for s in (1, -1):
        arrived(across(3 * s))
    for half in (0, 1):
        arrived(across(4), half)
    pl.semaphore_wait(tok.at[1], 1)

    def product(g):
        used = jnp.where(cnts_s[0, g] > 1, 1.0, 0.0).astype(F32)
        x = jnp.concatenate([xg[cols_s[0, g]], xg[cols_s[1, g]] * used], axis=1)
        hi, lo = split(x)
        o = lax.dot_general(
            jnp.concatenate([hi, lo], axis=0), mw[g], (((1,), (1,)), ((), ())),
            preferred_element_type=F32,
        )
        return o[:NV, :BS] + (o[:NV, BS:] + o[NV:, :BS])

    for i, d in enumerate(Q_ORDER):
        q = chip_of(*d)
        for k in range(2):
            pout[q, k] = product(4 * q + 2 * (1 - core) + k)
        cp = remote(pout.at[q], pin.at[q], p_send.at[i], p_recv.at[q], r, pair)
        cp.start()
        sends.append(cp)
    for i, d in enumerate(Q_ORDER):
        q = chip_of(*d)
        for k in range(2):
            sb[q, k] = product(4 * q + 2 * core + k)
        remote(pout.at[q], pin.at[q], p_send.at[i], p_recv.at[q], r, pair).wait_recv()
        for k in range(2):
            sb[q, k] = sb[q, k] + pin[q, k]
        if d != (0, 0):
            cp = remote(sb.at[q], rb.at[chip], s_send.at[i], s_recv.at[chip], r, q * 2 + core)
            cp.start()
            sends.append(cp)

    total = [sb[chip, 0], sb[chip, 1]]
    for d in Q_ORDER[:-1]:
        q = chip_of(*d)
        remote(sb.at[q], rb.at[q], s_send.at[0], s_recv.at[q], r, c).wait_recv()
        for k in range(2):
            total[k] = total[k] + rb[q, k]
    contrib = []
    sq = jnp.zeros((NV, BS), F32)
    for k in range(2):
        res = rhs_v[k] - total[k]
        resid[k] = res
        sq = sq + res * res
        hi, lo = split(res)
        o = lax.dot_general(
            jnp.concatenate([hi, lo], axis=0), rw[k],
            (((1,), (0,)), ((), ())), preferred_element_type=F32,
        )
        tmp[k] = o[:NV, :BS] + (o[:NV, BS:] + o[NV:, :BS])

    eye = diagonal()
    sq_row = jnp.sum(jnp.where(eye, jnp.sum(sq, axis=1, keepdims=True), 0.0), axis=0, keepdims=True)
    for k in range(2):
        for v in range(2):
            aout[pl.ds(2 * k + v, NC, stride=8), :] = tmp[k, pl.ds(v, NC, stride=2), :]
        aout[pl.ds(5 + k, NC, stride=8), :] = jnp.full((NC, BS), agg_s[k].astype(F32), F32)
    aout[pl.ds(4, NC, stride=8), :] = jnp.broadcast_to(sq_row, (NC, BS))
    aout[pl.ds(7, NC, stride=8), :] = jnp.zeros((NC, BS), F32)

    sqs[...] = jnp.broadcast_to(sq_row, (8, BS))

    def line(ref, j):
        return ref.at[pl.ds(pl.multiple_of(8 * j, 8), 1)]

    def tile(ref, j):
        return ref.at[pl.ds(pl.multiple_of(8 * j, 8), 8)]

    for d in range(1, NC):
        j = (c + d) % NC
        cp = remote(tile(aout, j), tile(ain, c), a_send.at[d], a_recv.at[c], r, j)
        cp.start()
        sends.append(cp)
    for d in range(NC):
        cp = remote(line(sqs, 0), line(sqa, c), o_send.at[d], o_recv.at[c], other, (c + d) % NC)
        cp.start()
        sends.append(cp)
    tile(ain, c)[...] = tile(aout, c)[...]

    who = lax.broadcasted_iota(jnp.int32, (NAGG, BS), 0).astype(F32)
    acc = [jnp.zeros((NAGG, BS), F32) for _ in range(2)]
    group_sq = jnp.zeros((1, BS), F32)
    for d in range(NC):
        j = (c + NC - d) % NC
        if d > 0:
            remote(tile(aout, j), tile(ain, j), a_send.at[0], a_recv.at[j], r, c).wait_recv()
        t = tile(ain, j)[...]
        for k in range(2):
            sel = who == t[5 + k:6 + k, :]
            for v in range(2):
                acc[v] = acc[v] + jnp.where(sel, t[2 * k + v:2 * k + v + 1, :], 0.0)
        group_sq = group_sq + t[4:5, :]

    def slot(j):
        return cbuf.at[pl.ds(pl.multiple_of(16 * j, 16), 16)]

    slot(c)[0:8, :] = acc[0]
    slot(c)[8:16, :] = acc[1]
    for d in range(1, NC):
        j = (c + d) % NC
        cp = remote(slot(c), slot(c), b_send.at[d], b_recv.at[c], r, j)
        cp.start()
        sends.append(cp)

    plane_sq = group_sq
    for d in range(NC):
        j = (c + NC - d) % NC
        remote(line(sqs, 0), line(sqa, j), o_send.at[0], o_recv.at[j], r, c).wait_recv()
        plane_sq = plane_sq + line(sqa, j)[...]
    tile(sqb, z)[...] = jnp.broadcast_to(plane_sq, (8, BS))
    for d in (4, 3, 5, 2, 6, 1, 7):
        cp = remote(line(sqb, z), line(sqb, z), q_send.at[d], q_recv.at[z], z_row(d), c)
        cp.start()
        sends.append(cp)

    for d in range(1, NZ):
        j = (z + d) % NZ
        remote(line(sqb, j), line(sqb, j), q_send.at[0], q_recv.at[j], r, c).wait_recv()
    for d in range(1, NC):
        j = (c + NC - d) % NC
        remote(slot(j), slot(j), b_send.at[0], b_recv.at[j], r, c).wait_recv()
    for cp in sends:
        cp.wait_send()


def finish(cbuf, sqb, resid, coarse_out, resid_out):
    all_sq = jnp.sum(sqb[pl.ds(0, NZ, stride=8), :], axis=0, keepdims=True)
    mean = all_sq * (1.0 / (NR * GR * BS)) + 1e-6
    mean_v = jnp.sum(jnp.where(diagonal(), jnp.broadcast_to(mean, (NV, BS)), 0.0), axis=1, keepdims=True)
    inv = jnp.broadcast_to(1.0 / jnp.sqrt(mean_v), (NV, BS))
    for a in range(NAGG):
        coarse_out[a] = cbuf[pl.ds(a, NV, stride=8), :] * inv
    resid_out[...] = resid[...]


def local(matrix, columns, counts, fine_guess, right_side, aggregate, restrict):
    dma = pltpu.SemaphoreType.DMA
    vmem = pl.BlockSpec(memory_space=pltpu.VMEM)
    parts = pl.pallas_call(
        kernel,
        out_shape=(
            pltpu.VMEM((NC * 16, BS), F32),
            pltpu.VMEM((NZ * 8, BS), F32),
            pltpu.VMEM((2, NV, BS), F32),
        ),
        in_specs=[pl.BlockSpec(memory_space=pltpu.HBM)] * 7,
        out_specs=(vmem,) * 3,
        scratch_shapes=[
            pltpu.VMEM((GR, KB, BS, BS), F32),
            pltpu.VMEM((GR, 2 * BS, KB * BS), BF16),
            pltpu.VMEM((2 * NR, NV, BS), F32),
            pltpu.VMEM((NQ, 2, NV, BS), F32),
            pltpu.VMEM((NQ, 2, NV, BS), F32),
            pltpu.VMEM((NQ, 2, NV, BS), F32),
            pltpu.VMEM((NQ, 2, NV, BS), F32),
            pltpu.VMEM((NC * 8, BS), F32),
            pltpu.VMEM((NC * 8, BS), F32),
            pltpu.VMEM((2, NV, BS), F32),
            pltpu.VMEM((2, BS, BS), F32),
            pltpu.VMEM((2, BS, 2 * BS), BF16),
            pltpu.VMEM((2, NV, BS), F32),
            pltpu.VMEM((8, BS), F32),
            pltpu.VMEM((NC * 8, BS), F32),
            pltpu.SMEM((KB, GR), jnp.int32),
            pltpu.SMEM((1, GR), jnp.int32),
            pltpu.SMEM((2,), jnp.int32),
            dma((CHUNKS,)), dma((6,)),
            dma((24,)), dma((2 * NR,)),
            dma((NQ,)), dma((NQ,)),
            dma((NQ,)), dma((NQ,)),
            dma((NC,)), dma((NC,)),
            dma((NC,)), dma((NC,)),
            dma((NC,)), dma((NC,)),
            dma((NZ,)), dma((NZ,)),
            pltpu.SemaphoreType.REGULAR((2,)),
        ],
        compiler_params=pltpu.CompilerParams(collective_id=0, has_side_effects=True, vmem_limit_bytes=60 * 2**20),
    )(matrix, columns.T, counts.T, fine_guess, right_side, aggregate, restrict)
    return pl.pallas_call(
        finish,
        out_shape=(
            jax.ShapeDtypeStruct((NAGG, NV, BS), F32),
            jax.ShapeDtypeStruct((2, NV, BS), F32),
        ),
        in_specs=[vmem] * 3,
        out_specs=(vmem,) * 2,
        compiler_params=pltpu.CompilerParams(vmem_limit_bytes=4 * 2**20),
    )(*parts)


def solution(mesh):
    in_specs = (
        P("row", "col", None, None),
        P("row", "col"),
        P("row", "col"),
        P(("col", "row"), None, None),
        P(("row", "col"), None, None),
        P(("row", "col")),
        P(("row", "col"), None, None),
    )
    out_specs = (P("row", None, None), P(("row", "col"), None, None))
    return jax.shard_map(local, mesh=mesh, in_specs=in_specs, out_specs=out_specs, check_vma=False)
```

```python
import jax
import jax.numpy as jnp
from jax import lax
from jax.experimental import pallas as pl
from jax.experimental.pallas import tpu as pltpu
from jax.sharding import PartitionSpec as P

MESH = pl.DeviceIdType.MESH
F32 = jnp.float32
BF16 = jnp.bfloat16

NR, NC = 16, 16
NZ = NR // 2
NQ = NC // 2
GR, KB, NV, BS = 32, 2, 32, 128
NAGG = 8
CHUNKS = 4
Q_ORDER = ((2, 1), (1, 1), (3, 1), (2, 0), (0, 1), (1, 0), (3, 0), (0, 0))


def split(x):
    hi = x.astype(BF16)
    return hi, (x - hi.astype(F32)).astype(BF16)


def diagonal():
    lane = lax.broadcasted_iota(jnp.int32, (NV, BS), 1)
    return lane == lax.broadcasted_iota(jnp.int32, (NV, BS), 0)


def kernel(
    mat, cols, cnts, xin, rhs, agg, rest, cbuf, sqb, resid,
    mraw, mw, xg, pout, pin, sb, rb, aout, ain, rhs_v, rest_v, rw, tmp, sqs, sqa,
    cols_s, cnts_s, agg_s,
    mat_sem, loc_sem, ag_send, ag_recv, p_send, p_recv, s_send, s_recv,
    a_send, a_recv, b_send, b_recv, o_send, o_recv, q_send, q_recv, tok,
):
    r = lax.axis_index("row")
    c = lax.axis_index("col")
    z, xl = r // 2, r % 2
    core, chip = c % 2, c // 2
    y, xh = chip // 2, chip % 2

    def remote(src, dst, ss, rs, row, col):
        return pltpu.make_async_remote_copy(
            src_ref=src, dst_ref=dst, send_sem=ss, recv_sem=rs,
            device_id=(row, col), device_id_type=MESH,
        )

    sends = []
    barrier = pltpu.get_barrier_semaphore()

    def z_row(d):
        return ((z + NZ + d) % NZ) * 2 + xl

    def chip_of(dy, dx):
        return ((y + dy) % 4) * 2 + (xh + dx) % 2

    def col_of(dy, dx):
        return chip_of(dy, dx) * 2 + core

    other = z * 2 + 1 - xl
    pair = chip * 2 + 1 - core
    near = [(z_row(d), c) for d in (2, -2, 1, -1)]
    near += [(other, c), (r, col_of(0, 1)), (r, col_of(1, 0)), (r, col_of(3, 0)), (r, pair)]
    for dev in near:
        pl.semaphore_signal(barrier, inc=1, device_id=dev, device_id_type=MESH)
    own_x = pltpu.make_async_copy(xin, xg.at[pl.ds(2 * r, 2)], loc_sem.at[0])
    own_x.start()
    per = GR // CHUNKS
    mats = [
        pltpu.make_async_copy(mat.at[pl.ds(k * per, per)], mraw.at[pl.ds(k * per, per)], mat_sem.at[k])
        for k in range(CHUNKS)
    ]
    for m in mats:
        m.start()
    smalls = [
        pltpu.make_async_copy(cols, cols_s, loc_sem.at[1]),
        pltpu.make_async_copy(cnts, cnts_s, loc_sem.at[2]),
        pltpu.make_async_copy(agg, agg_s, loc_sem.at[3]),
        pltpu.make_async_copy(rhs, rhs_v, loc_sem.at[4]),
        pltpu.make_async_copy(rest, rest_v, loc_sem.at[5]),
    ]
    for m in smalls:
        m.start()

    own_x.wait()
    pl.semaphore_wait(barrier, len(near))

    def ag(row, half, to_row):
        if half is None:
            ref, sem = xg.at[pl.ds(2 * row, 2)], 2 * row
        else:
            ref, sem = xg.at[pl.ds(2 * row + half, 1)], 2 * row + half
        return remote(ref, ref, ag_send.at[len(sends)], ag_recv.at[sem], to_row, c)

    def pass_on(row, half, *targets):
        for to_row in targets:
            cp = ag(row, half, to_row)
            cp.start()
            sends.append(cp)

    def arrived(row, half=None):
        ag(row, half, r).wait_recv()

    def across(d):
        return ((z + NZ + d) % NZ) * 2 + 1 - xl

    pass_on(r, None, other, z_row(2), z_row(-2), z_row(1), z_row(-1))
    for d in (2, -2, 1, -1):
        pl.semaphore_signal(tok.at[2], inc=1, device_id=(z_row(d), c), device_id_type=MESH)
    for dy in (1, 3):
        pl.semaphore_signal(tok.at[0], inc=1, device_id=(r, col_of(dy, 0)), device_id_type=MESH)
    arrived(other)
    pass_on(other, None, z_row(1), z_row(-1))
    pl.semaphore_wait(tok.at[2], 4)
    for s in (1, -1):
        far = z_row(-2 * s)
        arrived(far)
        pass_on(far, (1 - s) // 2, across(2 * s), z_row(2 * s))
        pass_on(far, None, across(s), z_row(s), other)
    pl.semaphore_wait(tok.at[0], 2)
    pl.semaphore_signal(tok.at[1], inc=1, device_id=(r, col_of(0, 1)), device_id_type=MESH)

    for k in range(CHUNKS):
        mats[k].wait()

        def parts(g, carry):
            for s in range(KB):
                hi, lo = split(mraw[g, s])
                mw[g, 0:BS, s * BS:(s + 1) * BS] = hi
                mw[g, BS:2 * BS, s * BS:(s + 1) * BS] = lo
            return carry

        lax.fori_loop(k * per, (k + 1) * per, parts, 0)
    for m in smalls:
        m.wait()
    for k in range(2):
        whi, wlo = split(rest_v[k])
        rw[k, :, 0:BS] = whi
        rw[k, :, BS:2 * BS] = wlo
    for s in (1, -1):
        arrived(z_row(s))
        arrived(across(s))
        arrived(across(2 * s))
        arrived(z_row(3 * s))
        arrived(across(3 * s))
    for half in (0, 1):
        arrived(z_row(4), half)
        arrived(across(4), half)
    pl.semaphore_wait(tok.at[1], 1)

    def product(g):
        used = jnp.where(cnts_s[0, g] > 1, 1.0, 0.0).astype(F32)
        x = jnp.concatenate([xg[cols_s[0, g]], xg[cols_s[1, g]] * used], axis=1)
        hi, lo = split(x)
        o = lax.dot_general(
            jnp.concatenate([hi, lo], axis=0), mw[g], (((1,), (1,)), ((), ())),
            preferred_element_type=F32,
        )
        return o[:NV, :BS] + (o[:NV, BS:] + o[NV:, :BS])

    for i, d in enumerate(Q_ORDER):
        q = chip_of(*d)
        for k in range(2):
            pout[q, k] = product(4 * q + 2 * (1 - core) + k)
        cp = remote(pout.at[q], pin.at[q], p_send.at[i], p_recv.at[q], r, pair)
        cp.start()
        sends.append(cp)
    for i, d in enumerate(Q_ORDER):
        q = chip_of(*d)
        for k in range(2):
            sb[q, k] = product(4 * q + 2 * core + k)
        remote(pout.at[q], pin.at[q], p_send.at[i], p_recv.at[q], r, pair).wait_recv()
        for k in range(2):
            sb[q, k] = sb[q, k] + pin[q, k]
        if d != (0, 0):
            cp = remote(sb.at[q], rb.at[chip], s_send.at[i], s_recv.at[chip], r, q * 2 + core)
            cp.start()
            sends.append(cp)

    total = [sb[chip, 0], sb[chip, 1]]
    for d in Q_ORDER[:-1]:
        q = chip_of(*d)
        remote(sb.at[q], rb.at[q], s_send.at[0], s_recv.at[q], r, c).wait_recv()
        for k in range(2):
            total[k] = total[k] + rb[q, k]
    contrib = []
    sq = jnp.zeros((NV, BS), F32)
    for k in range(2):
        res = rhs_v[k] - total[k]
        resid[k] = res
        sq = sq + res * res
        hi, lo = split(res)
        o = lax.dot_general(
            jnp.concatenate([hi, lo], axis=0), rw[k],
            (((1,), (0,)), ((), ())), preferred_element_type=F32,
        )
        tmp[k] = o[:NV, :BS] + (o[:NV, BS:] + o[NV:, :BS])

    eye = diagonal()
    sq_row = jnp.sum(jnp.where(eye, jnp.sum(sq, axis=1, keepdims=True), 0.0), axis=0, keepdims=True)
    for k in range(2):
        for v in range(2):
            aout[pl.ds(2 * k + v, NC, stride=8), :] = tmp[k, pl.ds(v, NC, stride=2), :]
        aout[pl.ds(5 + k, NC, stride=8), :] = jnp.full((NC, BS), agg_s[k].astype(F32), F32)
    aout[pl.ds(4, NC, stride=8), :] = jnp.broadcast_to(sq_row, (NC, BS))
    aout[pl.ds(7, NC, stride=8), :] = jnp.zeros((NC, BS), F32)

    sqs[...] = jnp.broadcast_to(sq_row, (8, BS))

    def line(ref, j):
        return ref.at[pl.ds(pl.multiple_of(8 * j, 8), 1)]

    def tile(ref, j):
        return ref.at[pl.ds(pl.multiple_of(8 * j, 8), 8)]

    for d in range(1, NC):
        j = (c + d) % NC
        cp = remote(tile(aout, j), tile(ain, c), a_send.at[d], a_recv.at[c], r, j)
        cp.start()
        sends.append(cp)
    for d in range(NC):
        cp = remote(line(sqs, 0), line(sqa, c), o_send.at[d], o_recv.at[c], other, (c + d) % NC)
        cp.start()
        sends.append(cp)
    tile(ain, c)[...] = tile(aout, c)[...]

    who = lax.broadcasted_iota(jnp.int32, (NAGG, BS), 0).astype(F32)
    acc = [jnp.zeros((NAGG, BS), F32) for _ in range(2)]
    group_sq = jnp.zeros((1, BS), F32)
    for d in range(NC):
        j = (c + NC - d) % NC
        if d > 0:
            remote(tile(aout, j), tile(ain, j), a_send.at[0], a_recv.at[j], r, c).wait_recv()
        t = tile(ain, j)[...]
        for k in range(2):
            sel = who == t[5 + k:6 + k, :]
            for v in range(2):
                acc[v] = acc[v] + jnp.where(sel, t[2 * k + v:2 * k + v + 1, :], 0.0)
        group_sq = group_sq + t[4:5, :]

    def slot(j):
        return cbuf.at[pl.ds(pl.multiple_of(16 * j, 16), 16)]

    slot(c)[0:8, :] = acc[0]
    slot(c)[8:16, :] = acc[1]
    for d in range(1, NC):
        j = (c + d) % NC
        cp = remote(slot(c), slot(c), b_send.at[d], b_recv.at[c], r, j)
        cp.start()
        sends.append(cp)

    plane_sq = group_sq
    for d in range(NC):
        j = (c + NC - d) % NC
        remote(line(sqs, 0), line(sqa, j), o_send.at[0], o_recv.at[j], r, c).wait_recv()
        plane_sq = plane_sq + line(sqa, j)[...]
    tile(sqb, z)[...] = jnp.broadcast_to(plane_sq, (8, BS))
    for d in (4, 3, 5, 2, 6, 1, 7):
        cp = remote(line(sqb, z), line(sqb, z), q_send.at[d], q_recv.at[z], z_row(d), c)
        cp.start()
        sends.append(cp)

    for d in range(1, NZ):
        j = (z + d) % NZ
        remote(line(sqb, j), line(sqb, j), q_send.at[0], q_recv.at[j], r, c).wait_recv()
    for d in range(1, NC):
        j = (c + NC - d) % NC
        remote(slot(j), slot(j), b_send.at[0], b_recv.at[j], r, c).wait_recv()
    for cp in sends:
        cp.wait_send()


def finish(cbuf, sqb, resid, coarse_out, resid_out):
    all_sq = jnp.sum(sqb[pl.ds(0, NZ, stride=8), :], axis=0, keepdims=True)
    mean = all_sq * (1.0 / (NR * GR * BS)) + 1e-6
    mean_v = jnp.sum(jnp.where(diagonal(), jnp.broadcast_to(mean, (NV, BS)), 0.0), axis=1, keepdims=True)
    inv = jnp.broadcast_to(1.0 / jnp.sqrt(mean_v), (NV, BS))
    for a in range(NAGG):
        coarse_out[a] = cbuf[pl.ds(a, NV, stride=8), :] * inv
    resid_out[...] = resid[...]


def local(matrix, columns, counts, fine_guess, right_side, aggregate, restrict):
    dma = pltpu.SemaphoreType.DMA
    vmem = pl.BlockSpec(memory_space=pltpu.VMEM)
    parts = pl.pallas_call(
        kernel,
        out_shape=(
            pltpu.VMEM((NC * 16, BS), F32),
            pltpu.VMEM((NZ * 8, BS), F32),
            pltpu.VMEM((2, NV, BS), F32),
        ),
        in_specs=[pl.BlockSpec(memory_space=pltpu.HBM)] * 7,
        out_specs=(vmem,) * 3,
        scratch_shapes=[
            pltpu.VMEM((GR, KB, BS, BS), F32),
            pltpu.VMEM((GR, 2 * BS, KB * BS), BF16),
            pltpu.VMEM((2 * NR, NV, BS), F32),
            pltpu.VMEM((NQ, 2, NV, BS), F32),
            pltpu.VMEM((NQ, 2, NV, BS), F32),
            pltpu.VMEM((NQ, 2, NV, BS), F32),
            pltpu.VMEM((NQ, 2, NV, BS), F32),
            pltpu.VMEM((NC * 8, BS), F32),
            pltpu.VMEM((NC * 8, BS), F32),
            pltpu.VMEM((2, NV, BS), F32),
            pltpu.VMEM((2, BS, BS), F32),
            pltpu.VMEM((2, BS, 2 * BS), BF16),
            pltpu.VMEM((2, NV, BS), F32),
            pltpu.VMEM((8, BS), F32),
            pltpu.VMEM((NC * 8, BS), F32),
            pltpu.SMEM((KB, GR), jnp.int32),
            pltpu.SMEM((1, GR), jnp.int32),
            pltpu.SMEM((2,), jnp.int32),
            dma((CHUNKS,)), dma((6,)),
            dma((24,)), dma((2 * NR,)),
            dma((NQ,)), dma((NQ,)),
            dma((NQ,)), dma((NQ,)),
            dma((NC,)), dma((NC,)),
            dma((NC,)), dma((NC,)),
            dma((NC,)), dma((NC,)),
            dma((NZ,)), dma((NZ,)),
            pltpu.SemaphoreType.REGULAR((3,)),
        ],
        compiler_params=pltpu.CompilerParams(collective_id=0, has_side_effects=True, vmem_limit_bytes=60 * 2**20),
    )(matrix, columns.T, counts.T, fine_guess, right_side, aggregate, restrict)
    return pl.pallas_call(
        finish,
        out_shape=(
            jax.ShapeDtypeStruct((NAGG, NV, BS), F32),
            jax.ShapeDtypeStruct((2, NV, BS), F32),
        ),
        in_specs=[vmem] * 3,
        out_specs=(vmem,) * 2,
        compiler_params=pltpu.CompilerParams(vmem_limit_bytes=4 * 2**20),
    )(*parts)


def solution(mesh):
    in_specs = (
        P("row", "col", None, None),
        P("row", "col"),
        P("row", "col"),
        P(("col", "row"), None, None),
        P(("row", "col"), None, None),
        P(("row", "col")),
        P(("row", "col"), None, None),
    )
    out_specs = (P("row", None, None), P(("row", "col"), None, None))
    return jax.shard_map(local, mesh=mesh, in_specs=in_specs, out_specs=out_specs, check_vma=False)
```

```python
import jax
import jax.numpy as jnp
from jax import lax
from jax.experimental import pallas as pl
from jax.experimental.pallas import tpu as pltpu
from jax.sharding import PartitionSpec as P

MESH = pl.DeviceIdType.MESH
F32 = jnp.float32
BF16 = jnp.bfloat16

NR, NC = 16, 16
NZ = NR // 2
NQ = NC // 2
GR, KB, NV, BS = 32, 2, 32, 128
NAGG = 8
CHUNKS = 4
Q_ORDER = ((2, 1), (1, 1), (3, 1), (2, 0), (0, 1), (1, 0), (3, 0), (0, 0))


def split(x):
    hi = x.astype(BF16)
    return hi, (x - hi.astype(F32)).astype(BF16)


def diagonal():
    lane = lax.broadcasted_iota(jnp.int32, (NV, BS), 1)
    return lane == lax.broadcasted_iota(jnp.int32, (NV, BS), 0)


def kernel(
    mat, cols, cnts, xin, rhs, agg, rest, cbuf, sqb, resid,
    mraw, mw, xg, pout, pin, sb, rb, aout, ain, rhs_v, rest_v, agg_v, rw, tmp, sqs, sqa,
    cols_s, cnts_s, agg_s,
    mat_sem, loc_sem, ag_send, ag_recv, p_send, p_recv, s_send, s_recv, e_send, e_recv,
    a_send, a_recv, b_send, b_recv, o_send, o_recv, q_send, q_recv, tok,
):
    r = lax.axis_index("row")
    c = lax.axis_index("col")
    z, xl = r // 2, r % 2
    core, chip = c % 2, c // 2
    y, xh = chip // 2, chip % 2

    def remote(src, dst, ss, rs, row, col):
        return pltpu.make_async_remote_copy(
            src_ref=src, dst_ref=dst, send_sem=ss, recv_sem=rs,
            device_id=(row, col), device_id_type=MESH,
        )

    sends = []
    barrier = pltpu.get_barrier_semaphore()

    def z_row(d):
        return ((z + NZ + d) % NZ) * 2 + xl

    def chip_of(dy, dx):
        return ((y + dy) % 4) * 2 + (xh + dx) % 2

    def col_of(dy, dx):
        return chip_of(dy, dx) * 2 + core

    other = z * 2 + 1 - xl
    pair = chip * 2 + 1 - core
    near = [(z_row(d), c) for d in (2, -2, 1, -1)]
    near += [(other, c), (r, col_of(0, 1)), (r, col_of(1, 0)), (r, col_of(3, 0)), (r, pair)]
    for dev in near:
        pl.semaphore_signal(barrier, inc=1, device_id=dev, device_id_type=MESH)
    own_x = pltpu.make_async_copy(xin, xg.at[pl.ds(2 * r, 2)], loc_sem.at[0])
    own_x.start()
    per = GR // CHUNKS
    mats = [
        pltpu.make_async_copy(mat.at[pl.ds(k * per, per)], mraw.at[pl.ds(k * per, per)], mat_sem.at[k])
        for k in range(CHUNKS)
    ]
    for m in mats:
        m.start()
    smalls = [
        pltpu.make_async_copy(cols, cols_s, loc_sem.at[1]),
        pltpu.make_async_copy(cnts, cnts_s, loc_sem.at[2]),
        pltpu.make_async_copy(agg, agg_s, loc_sem.at[3]),
        pltpu.make_async_copy(rhs, rhs_v.at[core], loc_sem.at[4]),
        pltpu.make_async_copy(rest, rest_v.at[core], loc_sem.at[5]),
    ]
    for m in smalls:
        m.start()

    own_x.wait()
    pl.semaphore_wait(barrier, len(near))

    def ag(row, half, to_row):
        if half is None:
            ref, sem = xg.at[pl.ds(2 * row, 2)], 2 * row
        else:
            ref, sem = xg.at[pl.ds(2 * row + half, 1)], 2 * row + half
        return remote(ref, ref, ag_send.at[len(sends)], ag_recv.at[sem], to_row, c)

    def pass_on(row, half, *targets):
        for to_row in targets:
            cp = ag(row, half, to_row)
            cp.start()
            sends.append(cp)

    def arrived(row, half=None):
        ag(row, half, r).wait_recv()

    def across(d):
        return ((z + NZ + d) % NZ) * 2 + 1 - xl

    pass_on(r, None, other, z_row(2), z_row(-2), z_row(1), z_row(-1))
    for d in (2, -2, 1, -1):
        pl.semaphore_signal(tok.at[2], inc=1, device_id=(z_row(d), c), device_id_type=MESH)
    for dy in (1, 3):
        pl.semaphore_signal(tok.at[0], inc=1, device_id=(r, col_of(dy, 0)), device_id_type=MESH)
    arrived(other)
    pass_on(other, None, z_row(1), z_row(-1))
    pl.semaphore_wait(tok.at[2], 4)
    for s in (1, -1):
        far = z_row(-2 * s)
        arrived(far)
        pass_on(far, (1 - s) // 2, across(2 * s), z_row(2 * s))
        pass_on(far, None, across(s), z_row(s), other)
    pl.semaphore_wait(tok.at[0], 2)
    pl.semaphore_signal(tok.at[1], inc=1, device_id=(r, col_of(0, 1)), device_id_type=MESH)

    for k in range(CHUNKS):
        mats[k].wait()

        def parts(g, carry):
            for s in range(KB):
                hi, lo = split(mraw[g, s])
                mw[g, 0:BS, s * BS:(s + 1) * BS] = hi
                mw[g, BS:2 * BS, s * BS:(s + 1) * BS] = lo
            return carry

        lax.fori_loop(k * per, (k + 1) * per, parts, 0)
    for m in smalls:
        m.wait()
    for k in range(2):
        agg_v[core, k] = jnp.full((8, BS), agg_s[k].astype(F32), F32)

    def hand_over(i, ref):
        return remote(ref.at[0], ref.at[0], e_send.at[i], e_recv.at[i], r, pair)

    handed = [hand_over(i, ref) for i, ref in enumerate((rhs_v, rest_v, agg_v))]

    @pl.when(core == 0)
    def _():
        for cp in handed:
            cp.start()

    @pl.when(core == 1)
    def _():
        for cp in handed:
            cp.wait_recv()
        for b in range(4):
            whi, wlo = split(rest_v[b // 2, b % 2])
            rw[b, :, 0:BS] = whi
            rw[b, :, BS:2 * BS] = wlo

    for s in (1, -1):
        arrived(z_row(s))
        arrived(across(s))
        arrived(across(2 * s))
        arrived(z_row(3 * s))
        arrived(across(3 * s))
    for half in (0, 1):
        arrived(z_row(4), half)
        arrived(across(4), half)
    pl.semaphore_wait(tok.at[1], 1)

    def product(g):
        used = jnp.where(cnts_s[0, g] > 1, 1.0, 0.0).astype(F32)
        x = jnp.concatenate([xg[cols_s[0, g]], xg[cols_s[1, g]] * used], axis=1)
        hi, lo = split(x)
        o = lax.dot_general(
            jnp.concatenate([hi, lo], axis=0), mw[g], (((1,), (1,)), ((), ())),
            preferred_element_type=F32,
        )
        return o[:NV, :BS] + (o[:NV, BS:] + o[NV:, :BS])

    for i, d in enumerate(Q_ORDER):
        q = chip_of(*d)
        for k in range(2):
            pout[q, k] = product(4 * q + 2 * (1 - core) + k)
        cp = remote(pout.at[q], pin.at[q], p_send.at[i], p_recv.at[q], r, pair)
        cp.start()
        sends.append(cp)
    for i, d in enumerate(Q_ORDER):
        q = chip_of(*d)
        for k in range(2):
            sb[q, k] = product(4 * q + 2 * core + k)
        remote(pout.at[q], pin.at[q], p_send.at[i], p_recv.at[q], r, pair).wait_recv()
        for k in range(2):
            sb[q, k] = sb[q, k] + pin[q, k]
        cp = remote(sb.at[q], rb.at[c], s_send.at[i], s_recv.at[c], r, q * 2 + 1)
        if d != (0, 0):
            cp.start()
            sends.append(cp)
    last = cp

    def line(ref, j):
        return ref.at[pl.ds(pl.multiple_of(8 * j, 8), 1)]

    def message(ref, j):
        return ref.at[pl.ds(pl.multiple_of(24 * j, 8), 24)]

    def slot(j):
        return cbuf.at[pl.ds(pl.multiple_of(32 * j, 32), 32)]

    def residual_to(col):
        return remote(tmp.at[pl.ds(0, 2)], resid, e_send.at[3], e_recv.at[3], r, col)

    @pl.when(core == 0)
    def _():
        last.start()
        for cp in handed + [last]:
            cp.wait_send()
        residual_to(pair).wait_recv()
        for d in range(NZ):
            remote(line(sqb, d), line(sqb, d), q_send.at[0], q_recv.at[d], r, c).wait_recv()
        for d in range(NQ):
            remote(slot(d), slot(d), b_send.at[0], b_recv.at[d], r, c).wait_recv()

    @pl.when(core == 1)
    def _():
        started = []

        def start(*args):
            cp = remote(*args)
            cp.start()
            started.append(cp)

        total = [None, None, sb[chip, 0], sb[chip, 1]]
        for d in Q_ORDER[::-1]:
            for half in (1, 0):
                if half == 1 and d == (0, 0):
                    continue
                j = chip_of(*d) * 2 + half
                remote(sb.at[0], rb.at[j], s_send.at[0], s_recv.at[j], r, c).wait_recv()
                for k in range(2):
                    b = 2 * half + k
                    total[b] = rb[j, k] if total[b] is None else total[b] + rb[j, k]
        sq = jnp.zeros((NV, BS), F32)
        for b in range(4):
            res = rhs_v[b // 2, b % 2] - total[b]
            if b < 2:
                tmp[b] = res
            else:
                resid[b - 2] = res
            sq = sq + res * res
            hi, lo = split(res)
            o = lax.dot_general(
                jnp.concatenate([hi, lo], axis=0), rw[b],
                (((1,), (0,)), ((), ())), preferred_element_type=F32,
            )
            tmp[2 + b] = o[:NV, :BS] + (o[:NV, BS:] + o[NV:, :BS])

        sq_row = jnp.sum(
            jnp.where(diagonal(), jnp.sum(sq, axis=1, keepdims=True), 0.0), axis=0, keepdims=True
        )
        for b in range(4):
            for v in range(4):
                aout[pl.ds(4 * b + v, NQ, stride=24), :] = tmp[2 + b, pl.ds(v, NQ, stride=4), :]
            aout[pl.ds(17 + b, NQ, stride=24), :] = agg_v[b // 2, b % 2]
        aout[pl.ds(16, NQ, stride=24), :] = jnp.broadcast_to(sq_row, (NQ, BS))
        for b in range(21, 24):
            aout[pl.ds(b, NQ, stride=24), :] = jnp.zeros((NQ, BS), F32)
        sqs[...] = jnp.broadcast_to(sq_row, (8, BS))

        for i, d in enumerate(Q_ORDER[:-1]):
            q = chip_of(*d)
            start(message(aout, q), message(ain, chip), a_send.at[i], a_recv.at[chip], r, q * 2 + 1)
        for i, d in enumerate(Q_ORDER):
            start(line(sqs, 0), line(sqa, chip), o_send.at[i], o_recv.at[chip], other, chip_of(*d) * 2 + 1)
        cp = residual_to(pair)
        cp.start()
        started.append(cp)

        who = lax.broadcasted_iota(jnp.int32, (NAGG, BS), 0).astype(F32)
        acc = [jnp.zeros((NAGG, BS), F32) for _ in range(4)]
        plane_sq = jnp.zeros((1, BS), F32)
        for d in Q_ORDER[::-1]:
            q = chip_of(*d)
            if d == (0, 0):
                t = message(aout, q)[...]
            else:
                remote(message(aout, q), message(ain, q), a_send.at[0], a_recv.at[q], r, c).wait_recv()
                t = message(ain, q)[...]
            for b in range(4):
                sel = who == t[17 + b:18 + b, :]
                for v in range(4):
                    acc[v] = acc[v] + jnp.where(sel, t[4 * b + v:4 * b + v + 1, :], 0.0)
            plane_sq = plane_sq + t[16:17, :]
        for v in range(4):
            slot(chip)[8 * v:8 * v + 8, :] = acc[v]
        for i, d in enumerate(Q_ORDER):
            q = chip_of(*d)
            start(slot(chip), slot(chip), b_send.at[2 * i], b_recv.at[chip], r, q * 2)
            if d != (0, 0):
                start(slot(chip), slot(chip), b_send.at[2 * i + 1], b_recv.at[chip], r, q * 2 + 1)

        for d in Q_ORDER[::-1]:
            q = chip_of(*d)
            remote(line(sqs, 0), line(sqa, q), o_send.at[0], o_recv.at[q], r, c).wait_recv()
            plane_sq = plane_sq + line(sqa, q)[...]
        line(sqb, z)[...] = plane_sq
        for i, d in enumerate((4, 3, 5, 2, 6, 1, 7, 0)):
            start(line(sqb, z), line(sqb, z), q_send.at[2 * i], q_recv.at[z], z_row(d), chip * 2)
            if d > 0:
                start(line(sqb, z), line(sqb, z), q_send.at[2 * i + 1], q_recv.at[z], z_row(d), c)
        for d in range(1, NZ):
            j = (z + d) % NZ
            remote(line(sqb, j), line(sqb, j), q_send.at[0], q_recv.at[j], r, c).wait_recv()
        for d in Q_ORDER[:-1]:
            q = chip_of(*d)
            remote(slot(q), slot(q), b_send.at[0], b_recv.at[q], r, c).wait_recv()
        for cp in started:
            cp.wait_send()

    for cp in sends:
        cp.wait_send()


def finish(cbuf, sqb, resid, coarse_out, resid_out):
    all_sq = jnp.sum(sqb[pl.ds(0, NZ, stride=8), :], axis=0, keepdims=True)
    mean = all_sq * (1.0 / (NR * GR * BS)) + 1e-6
    mean_v = jnp.sum(jnp.where(diagonal(), jnp.broadcast_to(mean, (NV, BS)), 0.0), axis=1, keepdims=True)
    inv = jnp.broadcast_to(1.0 / jnp.sqrt(mean_v), (NV, BS))
    for a in range(NAGG):
        coarse_out[a] = cbuf[pl.ds(a, NV, stride=8), :] * inv
    resid_out[...] = resid[...]


def local(matrix, columns, counts, fine_guess, right_side, aggregate, restrict):
    dma = pltpu.SemaphoreType.DMA
    vmem = pl.BlockSpec(memory_space=pltpu.VMEM)
    parts = pl.pallas_call(
        kernel,
        out_shape=(
            pltpu.VMEM((NC * 16, BS), F32),
            pltpu.VMEM((NZ * 8, BS), F32),
            pltpu.VMEM((2, NV, BS), F32),
        ),
        in_specs=[pl.BlockSpec(memory_space=pltpu.HBM)] * 7,
        out_specs=(vmem,) * 3,
        scratch_shapes=[
            pltpu.VMEM((GR, KB, BS, BS), F32),
            pltpu.VMEM((GR, 2 * BS, KB * BS), BF16),
            pltpu.VMEM((2 * NR, NV, BS), F32),
            pltpu.VMEM((NQ, 2, NV, BS), F32),
            pltpu.VMEM((NQ, 2, NV, BS), F32),
            pltpu.VMEM((NQ, 2, NV, BS), F32),
            pltpu.VMEM((NC, 2, NV, BS), F32),
            pltpu.VMEM((NQ * 24, BS), F32),
            pltpu.VMEM((NQ * 24, BS), F32),
            pltpu.VMEM((2, 2, NV, BS), F32),
            pltpu.VMEM((2, 2, BS, BS), F32),
            pltpu.VMEM((2, 2, 8, BS), F32),
            pltpu.VMEM((4, BS, 2 * BS), BF16),
            pltpu.VMEM((6, NV, BS), F32),
            pltpu.VMEM((8, BS), F32),
            pltpu.VMEM((NQ * 8, BS), F32),
            pltpu.SMEM((KB, GR), jnp.int32),
            pltpu.SMEM((1, GR), jnp.int32),
            pltpu.SMEM((2,), jnp.int32),
            dma((CHUNKS,)), dma((6,)),
            dma((24,)), dma((2 * NR,)),
            dma((NQ,)), dma((NQ,)),
            dma((NQ,)), dma((NC,)),
            dma((4,)), dma((4,)),
            dma((NQ,)), dma((NQ,)),
            dma((NC,)), dma((NQ,)),
            dma((NQ,)), dma((NQ,)),
            dma((NC,)), dma((NZ,)),
            pltpu.SemaphoreType.REGULAR((3,)),
        ],
        compiler_params=pltpu.CompilerParams(collective_id=0, has_side_effects=True, vmem_limit_bytes=60 * 2**20),
    )(matrix, columns.T, counts.T, fine_guess, right_side, aggregate, restrict)
    return pl.pallas_call(
        finish,
        out_shape=(
            jax.ShapeDtypeStruct((NAGG, NV, BS), F32),
            jax.ShapeDtypeStruct((2, NV, BS), F32),
        ),
        in_specs=[vmem] * 3,
        out_specs=(vmem,) * 2,
        compiler_params=pltpu.CompilerParams(vmem_limit_bytes=4 * 2**20),
    )(*parts)


def solution(mesh):
    in_specs = (
        P("row", "col", None, None),
        P("row", "col"),
        P("row", "col"),
        P(("col", "row"), None, None),
        P(("row", "col"), None, None),
        P(("row", "col")),
        P(("row", "col"), None, None),
    )
    out_specs = (P("row", None, None), P(("row", "col"), None, None))
    return jax.shard_map(local, mesh=mesh, in_specs=in_specs, out_specs=out_specs, check_vma=False)
```

```python
import jax
import jax.numpy as jnp
from jax import lax
from jax.experimental import pallas as pl
from jax.experimental.pallas import tpu as pltpu
from jax.sharding import PartitionSpec as P

MESH = pl.DeviceIdType.MESH
F32 = jnp.float32
BF16 = jnp.bfloat16

NR, NC = 16, 16
NZ = NR // 2
NQ = NC // 2
GR, KB, NV, BS = 32, 2, 32, 128
NAGG = 8
CHUNKS = 4
Q_ORDER = ((2, 1), (2, 0), (1, 1), (3, 1), (0, 1), (1, 0), (3, 0), (0, 0))
BATCH1 = 4
BATCH2 = 4


def split(x):
    hi = x.astype(BF16)
    return hi, (x - hi.astype(F32)).astype(BF16)


def diagonal():
    lane = lax.broadcasted_iota(jnp.int32, (NV, BS), 1)
    return lane == lax.broadcasted_iota(jnp.int32, (NV, BS), 0)


def kernel(
    mat, cols, cnts, xin, rhs, agg, rest, cbuf, sqb, resid,
    mraw, mw, xg, pout, pin, sb, rb, aout, ain, rhs_v, rest_v, agg_v, rw, tmp, sqs, sqa,
    cols_s, cnts_s, agg_s,
    mat_sem, loc_sem, ag_send, ag_recv, p_send, p_recv, s_send, s_recv, e_send, e_recv,
    a_send, a_recv, b_send, b_recv, o_send, o_recv, q_send, q_recv, tok,
):
    r = lax.axis_index("row")
    c = lax.axis_index("col")
    z, xl = r // 2, r % 2
    core, chip = c % 2, c // 2
    y, xh = chip // 2, chip % 2

    def remote(src, dst, ss, rs, row, col):
        return pltpu.make_async_remote_copy(
            src_ref=src, dst_ref=dst, send_sem=ss, recv_sem=rs,
            device_id=(row, col), device_id_type=MESH,
        )

    sends = []
    barrier = pltpu.get_barrier_semaphore()

    def z_row(d):
        return ((z + NZ + d) % NZ) * 2 + xl

    def chip_of(dy, dx):
        return ((y + dy) % 4) * 2 + (xh + dx) % 2

    def col_of(dy, dx):
        return chip_of(dy, dx) * 2 + core

    other = z * 2 + 1 - xl
    pair = chip * 2 + 1 - core
    near = [(z_row(d), c) for d in (2, -2, 1, -1)]
    near += [(other, c), (r, col_of(0, 1)), (r, col_of(1, 0)), (r, col_of(3, 0)), (r, pair)]
    for dev in near:
        pl.semaphore_signal(barrier, inc=1, device_id=dev, device_id_type=MESH)
    own_x = pltpu.make_async_copy(xin, xg.at[pl.ds(2 * r, 2)], loc_sem.at[0])
    own_x.start()
    per = GR // CHUNKS
    mats = [
        pltpu.make_async_copy(mat.at[pl.ds(k * per, per)], mraw.at[pl.ds(k * per, per)], mat_sem.at[k])
        for k in range(CHUNKS)
    ]
    for m in mats:
        m.start()
    smalls = [
        pltpu.make_async_copy(cols, cols_s, loc_sem.at[1]),
        pltpu.make_async_copy(cnts, cnts_s, loc_sem.at[2]),
        pltpu.make_async_copy(agg, agg_s, loc_sem.at[3]),
        pltpu.make_async_copy(rhs, rhs_v.at[core], loc_sem.at[4]),
        pltpu.make_async_copy(rest, rest_v.at[core], loc_sem.at[5]),
    ]
    for m in smalls:
        m.start()

    own_x.wait()
    pl.semaphore_wait(barrier, len(near))

    def ag(row, half, to_row):
        if half is None:
            ref, sem = xg.at[pl.ds(2 * row, 2)], 2 * row
        else:
            ref, sem = xg.at[pl.ds(2 * row + half, 1)], 2 * row + half
        return remote(ref, ref, ag_send.at[len(sends)], ag_recv.at[sem], to_row, c)

    def pass_on(row, half, *targets):
        for to_row in targets:
            cp = ag(row, half, to_row)
            cp.start()
            sends.append(cp)

    def arrived(row, half=None):
        ag(row, half, r).wait_recv()

    def across(d):
        return ((z + NZ + d) % NZ) * 2 + 1 - xl

    pass_on(r, None, other, z_row(2), z_row(-2), z_row(1), z_row(-1))
    for d in (2, -2, 1, -1):
        pl.semaphore_signal(tok.at[2], inc=1, device_id=(z_row(d), c), device_id_type=MESH)
    for dy in (1, 3):
        pl.semaphore_signal(tok.at[0], inc=1, device_id=(r, col_of(dy, 0)), device_id_type=MESH)
    arrived(other)
    pass_on(other, None, z_row(1), z_row(-1))
    pl.semaphore_wait(tok.at[2], 4)
    for s in (1, -1):
        far = z_row(-2 * s)
        arrived(far)
        pass_on(far, (1 - s) // 2, across(2 * s), z_row(2 * s))
        pass_on(far, None, across(s), z_row(s), other)
    pl.semaphore_wait(tok.at[0], 2)
    pl.semaphore_signal(tok.at[1], inc=1, device_id=(r, col_of(0, 1)), device_id_type=MESH)

    for k in range(CHUNKS):
        mats[k].wait()

        def parts(g, carry):
            for s in range(KB):
                hi, lo = split(mraw[g, s].T)
                mw[g, s * BS:(s + 1) * BS, 0:BS] = hi
                mw[g, s * BS:(s + 1) * BS, BS:2 * BS] = lo
            return carry

        lax.fori_loop(k * per, (k + 1) * per, parts, 0, unroll=4)
    for m in smalls:
        m.wait()
    for k in range(2):
        agg_v[core, k] = jnp.full((8, BS), agg_s[k].astype(F32), F32)

    def hand_over(i, ref):
        return remote(ref.at[0], ref.at[0], e_send.at[i], e_recv.at[i], r, pair)

    handed = [hand_over(i, ref) for i, ref in enumerate((rhs_v, rest_v, agg_v))]

    @pl.when(core == 0)
    def _():
        for cp in handed:
            cp.start()

    @pl.when(core == 1)
    def _():
        for cp in handed:
            cp.wait_recv()
        for b in range(4):
            whi, wlo = split(rest_v[b // 2, b % 2])
            rw[b, :, 0:BS] = whi
            rw[b, :, BS:2 * BS] = wlo

    for s in (1, -1):
        arrived(z_row(s))
        arrived(across(s))
        arrived(across(2 * s))
        arrived(z_row(3 * s))
        arrived(across(3 * s))
    for half in (0, 1):
        arrived(z_row(4), half)
        arrived(across(4), half)
    pl.semaphore_wait(tok.at[1], 1)

    def product(g):
        used = jnp.where(cnts_s[0, g] > 1, 1.0, 0.0).astype(F32)
        x = jnp.concatenate([xg[cols_s[0, g]], xg[cols_s[1, g]] * used], axis=1)
        hi, lo = split(x)
        o = lax.dot_general(
            jnp.concatenate([hi, lo], axis=0), mw[g], (((1,), (0,)), ((), ())),
            preferred_element_type=F32,
        )
        return o[:NV, :BS] + (o[:NV, BS:] + o[NV:, :BS])

    for first in range(0, NQ, BATCH1):
        for d in Q_ORDER[first:first + BATCH1]:
            q = chip_of(*d)
            for k in range(2):
                pout[q, k] = product(4 * q + 2 * (1 - core) + k)
        for i in range(first, first + BATCH1):
            q = chip_of(*Q_ORDER[i])
            cp = remote(pout.at[q], pin.at[q], p_send.at[i], p_recv.at[q], r, pair)
            cp.start()
            sends.append(cp)
    for first in range(0, NQ, BATCH2):
        for d in Q_ORDER[first:first + BATCH2]:
            q = chip_of(*d)
            for k in range(2):
                sb[q, k] = product(4 * q + 2 * core + k)
        for i in range(first, first + BATCH2):
            q = chip_of(*Q_ORDER[i])
            remote(pout.at[q], pin.at[q], p_send.at[i], p_recv.at[q], r, pair).wait_recv()
            for k in range(2):
                sb[q, k] = sb[q, k] + pin[q, k]
            cp = remote(sb.at[q], rb.at[c], s_send.at[i], s_recv.at[c], r, q * 2 + 1)
            if i < NQ - 1:
                cp.start()
                sends.append(cp)
    last = cp

    def line(ref, j):
        return ref.at[pl.ds(pl.multiple_of(8 * j, 8), 1)]

    def message(ref, j):
        return ref.at[pl.ds(pl.multiple_of(24 * j, 8), 24)]

    def slot(j):
        return cbuf.at[pl.ds(pl.multiple_of(32 * j, 32), 32)]

    def residual_to(col):
        return remote(tmp.at[pl.ds(0, 2)], resid, e_send.at[3], e_recv.at[3], r, col)

    @pl.when(core == 0)
    def _():
        last.start()
        for cp in handed + [last]:
            cp.wait_send()
        residual_to(pair).wait_recv()
        for d in range(NZ):
            remote(line(sqb, d), line(sqb, d), q_send.at[0], q_recv.at[d], r, c).wait_recv()
        for d in range(NQ):
            remote(slot(d), slot(d), b_send.at[0], b_recv.at[d], r, c).wait_recv()

    @pl.when(core == 1)
    def _():
        started = []

        def start(*args):
            cp = remote(*args)
            cp.start()
            started.append(cp)

        total = [None, None, sb[chip, 0], sb[chip, 1]]
        for d in Q_ORDER[::-1]:
            for half in (1, 0):
                if half == 1 and d == (0, 0):
                    continue
                j = chip_of(*d) * 2 + half
                remote(sb.at[0], rb.at[j], s_send.at[0], s_recv.at[j], r, c).wait_recv()
                for k in range(2):
                    b = 2 * half + k
                    total[b] = rb[j, k] if total[b] is None else total[b] + rb[j, k]
        sq = jnp.zeros((NV, BS), F32)
        for b in range(4):
            res = rhs_v[b // 2, b % 2] - total[b]
            if b < 2:
                tmp[b] = res
            else:
                resid[b - 2] = res
            sq = sq + res * res
            hi, lo = split(res)
            o = lax.dot_general(
                jnp.concatenate([hi, lo], axis=0), rw[b],
                (((1,), (0,)), ((), ())), preferred_element_type=F32,
            )
            tmp[2 + b] = o[:NV, :BS] + (o[:NV, BS:] + o[NV:, :BS])

        sq_row = jnp.sum(
            jnp.where(diagonal(), jnp.sum(sq, axis=1, keepdims=True), 0.0), axis=0, keepdims=True
        )
        for b in range(4):
            for v in range(4):
                aout[pl.ds(4 * b + v, NQ, stride=24), :] = tmp[2 + b, pl.ds(v, NQ, stride=4), :]
            aout[pl.ds(17 + b, NQ, stride=24), :] = agg_v[b // 2, b % 2]
        aout[pl.ds(16, NQ, stride=24), :] = jnp.broadcast_to(sq_row, (NQ, BS))
        for b in range(21, 24):
            aout[pl.ds(b, NQ, stride=24), :] = jnp.zeros((NQ, BS), F32)
        sqs[...] = jnp.broadcast_to(sq_row, (8, BS))

        for i, d in enumerate(Q_ORDER[:-1]):
            q = chip_of(*d)
            start(message(aout, q), message(ain, chip), a_send.at[i], a_recv.at[chip], r, q * 2 + 1)
        for i, d in enumerate(Q_ORDER):
            start(line(sqs, 0), line(sqa, chip), o_send.at[i], o_recv.at[chip], other, chip_of(*d) * 2 + 1)
        cp = residual_to(pair)
        cp.start()
        started.append(cp)

        who = lax.broadcasted_iota(jnp.int32, (NAGG, BS), 0).astype(F32)
        acc = [jnp.zeros((NAGG, BS), F32) for _ in range(4)]
        plane_sq = jnp.zeros((1, BS), F32)
        for d in Q_ORDER[::-1]:
            q = chip_of(*d)
            if d == (0, 0):
                t = message(aout, q)[...]
            else:
                remote(message(aout, q), message(ain, q), a_send.at[0], a_recv.at[q], r, c).wait_recv()
                t = message(ain, q)[...]
            for b in range(4):
                sel = who == t[17 + b:18 + b, :]
                for v in range(4):
                    acc[v] = acc[v] + jnp.where(sel, t[4 * b + v:4 * b + v + 1, :], 0.0)
            plane_sq = plane_sq + t[16:17, :]
        for v in range(4):
            slot(chip)[8 * v:8 * v + 8, :] = acc[v]
        for i, d in enumerate(Q_ORDER[:-1]):
            start(slot(chip), slot(chip), b_send.at[2 * i + 1], b_recv.at[chip], r, chip_of(*d) * 2 + 1)
        for i, d in enumerate(Q_ORDER):
            start(slot(chip), slot(chip), b_send.at[2 * i], b_recv.at[chip], r, chip_of(*d) * 2)

        for d in Q_ORDER[::-1]:
            q = chip_of(*d)
            remote(line(sqs, 0), line(sqa, q), o_send.at[0], o_recv.at[q], r, c).wait_recv()
            plane_sq = plane_sq + line(sqa, q)[...]
        line(sqb, z)[...] = plane_sq
        for i, d in enumerate((4, 3, 5, 2, 6, 1, 7, 0)):
            start(line(sqb, z), line(sqb, z), q_send.at[2 * i], q_recv.at[z], z_row(d), chip * 2)
            if d > 0:
                start(line(sqb, z), line(sqb, z), q_send.at[2 * i + 1], q_recv.at[z], z_row(d), c)
        for d in range(1, NZ):
            j = (z + d) % NZ
            remote(line(sqb, j), line(sqb, j), q_send.at[0], q_recv.at[j], r, c).wait_recv()
        for d in Q_ORDER[:-1]:
            q = chip_of(*d)
            remote(slot(q), slot(q), b_send.at[0], b_recv.at[q], r, c).wait_recv()
        for cp in started:
            cp.wait_send()

    for cp in sends:
        cp.wait_send()


def finish(cbuf, sqb, resid, coarse_out, resid_out):
    all_sq = jnp.sum(sqb[pl.ds(0, NZ, stride=8), :], axis=0, keepdims=True)
    mean = all_sq * (1.0 / (NR * GR * BS)) + 1e-6
    mean_v = jnp.sum(jnp.where(diagonal(), jnp.broadcast_to(mean, (NV, BS)), 0.0), axis=1, keepdims=True)
    inv = jnp.broadcast_to(1.0 / jnp.sqrt(mean_v), (NV, BS))
    for a in range(NAGG):
        coarse_out[a] = cbuf[pl.ds(a, NV, stride=8), :] * inv
    resid_out[...] = resid[...]


def local(matrix, columns, counts, fine_guess, right_side, aggregate, restrict):
    dma = pltpu.SemaphoreType.DMA
    vmem = pl.BlockSpec(memory_space=pltpu.VMEM)
    parts = pl.pallas_call(
        kernel,
        out_shape=(
            pltpu.VMEM((NC * 16, BS), F32),
            pltpu.VMEM((NZ * 8, BS), F32),
            pltpu.VMEM((2, NV, BS), F32),
        ),
        in_specs=[pl.BlockSpec(memory_space=pltpu.HBM)] * 7,
        out_specs=(vmem,) * 3,
        scratch_shapes=[
            pltpu.VMEM((GR, KB, BS, BS), F32),
            pltpu.VMEM((GR, 2 * BS, KB * BS), BF16),
            pltpu.VMEM((2 * NR, NV, BS), F32),
            pltpu.VMEM((NQ, 2, NV, BS), F32),
            pltpu.VMEM((NQ, 2, NV, BS), F32),
            pltpu.VMEM((NQ, 2, NV, BS), F32),
            pltpu.VMEM((NC, 2, NV, BS), F32),
            pltpu.VMEM((NQ * 24, BS), F32),
            pltpu.VMEM((NQ * 24, BS), F32),
            pltpu.VMEM((2, 2, NV, BS), F32),
            pltpu.VMEM((2, 2, BS, BS), F32),
            pltpu.VMEM((2, 2, 8, BS), F32),
            pltpu.VMEM((4, BS, 2 * BS), BF16),
            pltpu.VMEM((6, NV, BS), F32),
            pltpu.VMEM((8, BS), F32),
            pltpu.VMEM((NQ * 8, BS), F32),
            pltpu.SMEM((KB, GR), jnp.int32),
            pltpu.SMEM((1, GR), jnp.int32),
            pltpu.SMEM((2,), jnp.int32),
            dma((CHUNKS,)), dma((6,)),
            dma((24,)), dma((2 * NR,)),
            dma((NQ,)), dma((NQ,)),
            dma((NQ,)), dma((NC,)),
            dma((4,)), dma((4,)),
            dma((NQ,)), dma((NQ,)),
            dma((NC,)), dma((NQ,)),
            dma((NQ,)), dma((NQ,)),
            dma((NC,)), dma((NZ,)),
            pltpu.SemaphoreType.REGULAR((3,)),
        ],
        compiler_params=pltpu.CompilerParams(collective_id=0, has_side_effects=True, vmem_limit_bytes=60 * 2**20),
    )(matrix, columns.T, counts.T, fine_guess, right_side, aggregate, restrict)
    return pl.pallas_call(
        finish,
        out_shape=(
            jax.ShapeDtypeStruct((NAGG, NV, BS), F32),
            jax.ShapeDtypeStruct((2, NV, BS), F32),
        ),
        in_specs=[vmem] * 3,
        out_specs=(vmem,) * 2,
        compiler_params=pltpu.CompilerParams(vmem_limit_bytes=4 * 2**20),
    )(*parts)


def solution(mesh):
    in_specs = (
        P("row", "col", None, None),
        P("row", "col"),
        P("row", "col"),
        P(("col", "row"), None, None),
        P(("row", "col"), None, None),
        P(("row", "col")),
        P(("row", "col"), None, None),
    )
    out_specs = (P("row", None, None), P(("row", "col"), None, None))
    return jax.shard_map(local, mesh=mesh, in_specs=in_specs, out_specs=out_specs, check_vma=False)
```

```python
import jax
import jax.numpy as jnp
from jax import lax
from jax.experimental import pallas as pl
from jax.experimental.pallas import tpu as pltpu
from jax.sharding import PartitionSpec as P

MESH = pl.DeviceIdType.MESH
F32 = jnp.float32
BF16 = jnp.bfloat16

NR, NC = 16, 16
NZ = NR // 2
NQ = NC // 2
GR, KB, NV, BS = 32, 2, 32, 128
NAGG = 8
CHUNKS = 4
Q_ORDER = ((2, 1), (2, 0), (1, 1), (3, 1), (0, 1), (1, 0), (3, 0), (0, 0))
BATCH1 = 4
BATCH2 = 4


def split(x):
    hi = x.astype(BF16)
    return hi, (x - hi.astype(F32)).astype(BF16)


def diagonal():
    lane = lax.broadcasted_iota(jnp.int32, (NV, BS), 1)
    return lane == lax.broadcasted_iota(jnp.int32, (NV, BS), 0)


def kernel(
    mat, cols, cnts, xin, rhs, agg, rest, cbuf, sqb, resid,
    mraw, mw, xg, pout, pin, sb, rb, aout, ain, rhs_v, rest_v, agg_v, rw, tmp, sqs, sqa,
    cols_s, cnts_s, agg_s,
    mat_sem, loc_sem, ag_send, ag_recv, p_send, p_recv, s_send, s_recv, e_send, e_recv,
    a_send, a_recv, b_send, b_recv, o_send, o_recv, q_send, q_recv, tok,
):
    r = lax.axis_index("row")
    c = lax.axis_index("col")
    z, xl = r // 2, r % 2
    core, chip = c % 2, c // 2
    y, xh = chip // 2, chip % 2

    def remote(src, dst, ss, rs, row, col):
        return pltpu.make_async_remote_copy(
            src_ref=src, dst_ref=dst, send_sem=ss, recv_sem=rs,
            device_id=(row, col), device_id_type=MESH,
        )

    sends = []
    barrier = pltpu.get_barrier_semaphore()

    def z_row(d):
        return ((z + NZ + d) % NZ) * 2 + xl

    def chip_of(dy, dx):
        return ((y + dy) % 4) * 2 + (xh + dx) % 2

    def col_of(dy, dx):
        return chip_of(dy, dx) * 2 + core

    other = z * 2 + 1 - xl
    pair = chip * 2 + 1 - core
    near = [(z_row(d), c) for d in (2, -2, 1, -1)]
    near += [(other, c), (r, col_of(0, 1)), (r, col_of(1, 0)), (r, col_of(3, 0)), (r, pair)]
    for dev in near:
        pl.semaphore_signal(barrier, inc=1, device_id=dev, device_id_type=MESH)
    own_x = pltpu.make_async_copy(xin, xg.at[pl.ds(2 * r, 2)], loc_sem.at[0])
    own_x.start()
    per = GR // CHUNKS
    mats = [
        pltpu.make_async_copy(mat.at[pl.ds(k * per, per)], mraw.at[pl.ds(k * per, per)], mat_sem.at[k])
        for k in range(CHUNKS)
    ]
    for m in mats:
        m.start()
    smalls = [
        pltpu.make_async_copy(cols, cols_s, loc_sem.at[1]),
        pltpu.make_async_copy(cnts, cnts_s, loc_sem.at[2]),
        pltpu.make_async_copy(agg, agg_s, loc_sem.at[3]),
        pltpu.make_async_copy(rhs, rhs_v.at[core], loc_sem.at[4]),
        pltpu.make_async_copy(rest, rest_v.at[core], loc_sem.at[5]),
    ]
    for m in smalls:
        m.start()

    own_x.wait()
    pl.semaphore_wait(barrier, len(near))

    def ag(row, half, to_row):
        if half is None:
            ref, sem = xg.at[pl.ds(2 * row, 2)], 2 * row
        else:
            ref, sem = xg.at[pl.ds(2 * row + half, 1)], 2 * row + half
        return remote(ref, ref, ag_send.at[len(sends)], ag_recv.at[sem], to_row, c)

    def pass_on(row, half, *targets):
        for to_row in targets:
            cp = ag(row, half, to_row)
            cp.start()
            sends.append(cp)

    def arrived(row, half=None):
        ag(row, half, r).wait_recv()

    def across(d):
        return ((z + NZ + d) % NZ) * 2 + 1 - xl

    pass_on(r, None, other, z_row(2), z_row(-2), z_row(1), z_row(-1))
    for d in (2, -2, 1, -1):
        pl.semaphore_signal(tok.at[2], inc=1, device_id=(z_row(d), c), device_id_type=MESH)
    for dy in (1, 3):
        pl.semaphore_signal(tok.at[0], inc=1, device_id=(r, col_of(dy, 0)), device_id_type=MESH)
    arrived(other)
    pass_on(other, None, z_row(1), z_row(-1))
    pl.semaphore_wait(tok.at[2], 4)
    for s in (1, -1):
        far = z_row(-2 * s)
        arrived(far)
        pass_on(far, (1 - s) // 2, across(2 * s), z_row(2 * s))
        pass_on(far, None, across(s), z_row(s), other)
    pl.semaphore_wait(tok.at[0], 2)
    pl.semaphore_signal(tok.at[1], inc=1, device_id=(r, col_of(0, 1)), device_id_type=MESH)

    for k in range(CHUNKS):
        mats[k].wait()

        def parts(g, carry):
            for s in range(KB):
                hi, lo = split(mraw[g, s].T)
                mw[g, s * BS:(s + 1) * BS, 0:BS] = hi
                mw[g, s * BS:(s + 1) * BS, BS:2 * BS] = lo
            return carry

        lax.fori_loop(k * per, (k + 1) * per, parts, 0, unroll=4)
    for m in smalls:
        m.wait()
    for k in range(2):
        agg_v[core, k] = jnp.full((8, BS), agg_s[k].astype(F32), F32)

    def hand_over(i, ref):
        return remote(ref.at[0], ref.at[0], e_send.at[i], e_recv.at[i], r, pair)

    handed = [hand_over(i, ref) for i, ref in enumerate((rhs_v, rest_v, agg_v))]

    @pl.when(core == 0)
    def _():
        for cp in handed:
            cp.start()

    @pl.when(core == 1)
    def _():
        for cp in handed:
            cp.wait_recv()
        for b in range(4):
            whi, wlo = split(rest_v[b // 2, b % 2])
            rw[b, :, 0:BS] = whi
            rw[b, :, BS:2 * BS] = wlo

    for s in (1, -1):
        arrived(z_row(s))
        arrived(across(s))
        arrived(across(2 * s))
        arrived(z_row(3 * s))
        arrived(across(3 * s))
    for half in (0, 1):
        arrived(z_row(4), half)
        arrived(across(4), half)
    pl.semaphore_wait(tok.at[1], 1)

    def product(g):
        used = jnp.where(cnts_s[0, g] > 1, 1.0, 0.0).astype(F32)
        x = jnp.concatenate([xg[cols_s[0, g]], xg[cols_s[1, g]] * used], axis=1)
        hi, lo = split(x)
        o = lax.dot_general(
            jnp.concatenate([hi, lo], axis=0), mw[g], (((1,), (0,)), ((), ())),
            preferred_element_type=F32,
        )
        return o[:NV, :BS] + (o[:NV, BS:] + o[NV:, :BS])

    for first in range(0, NQ, BATCH1):
        for d in Q_ORDER[first:first + BATCH1]:
            q = chip_of(*d)
            for k in range(2):
                pout[q, k] = product(4 * q + 2 * (1 - core) + k)
        for i in range(first, first + BATCH1):
            q = chip_of(*Q_ORDER[i])
            cp = remote(pout.at[q], pin.at[q], p_send.at[i], p_recv.at[q], r, pair)
            cp.start()
            sends.append(cp)
    for first in range(0, NQ, BATCH2):
        for d in Q_ORDER[first:first + BATCH2]:
            q = chip_of(*d)
            for k in range(2):
                sb[q, k] = product(4 * q + 2 * core + k)
        for i in range(first, first + BATCH2):
            q = chip_of(*Q_ORDER[i])
            remote(pout.at[q], pin.at[q], p_send.at[i], p_recv.at[q], r, pair).wait_recv()
            for k in range(2):
                sb[q, k] = sb[q, k] + pin[q, k]
            cp = remote(sb.at[q], rb.at[c], s_send.at[i], s_recv.at[c], r, q * 2 + 1)
            if i < NQ - 1:
                cp.start()
                sends.append(cp)
    last = cp

    def line(ref, j):
        return ref.at[pl.ds(pl.multiple_of(8 * j, 8), 1)]

    def message(ref, j):
        return ref.at[pl.ds(pl.multiple_of(24 * j, 8), 24)]

    def slot(j):
        return cbuf.at[pl.ds(pl.multiple_of(32 * j, 32), 32)]

    def residual_to(col):
        return remote(tmp.at[pl.ds(0, 2)], resid, e_send.at[3], e_recv.at[3], r, col)

    @pl.when(core == 0)
    def _():
        last.start()
        for cp in handed + [last]:
            cp.wait_send()
        residual_to(pair).wait_recv()
        for d in range(NZ):
            remote(line(sqb, d), line(sqb, d), q_send.at[0], q_recv.at[d], r, c).wait_recv()
        for d in range(NQ):
            remote(slot(d), slot(d), b_send.at[0], b_recv.at[d], r, c).wait_recv()

    @pl.when(core == 1)
    def _():
        started = []

        def start(*args):
            cp = remote(*args)
            cp.start()
            started.append(cp)

        total = [None, None, sb[chip, 0], sb[chip, 1]]
        for d in Q_ORDER[::-1]:
            for half in (1, 0):
                if half == 1 and d == (0, 0):
                    continue
                j = chip_of(*d) * 2 + half
                remote(sb.at[0], rb.at[j], s_send.at[0], s_recv.at[j], r, c).wait_recv()
                for k in range(2):
                    b = 2 * half + k
                    total[b] = rb[j, k] if total[b] is None else total[b] + rb[j, k]
        sq = jnp.zeros((NV, BS), F32)
        for b in range(4):
            res = rhs_v[b // 2, b % 2] - total[b]
            if b < 2:
                tmp[b] = res
            else:
                resid[b - 2] = res
            sq = sq + res * res
            hi, lo = split(res)
            o = lax.dot_general(
                jnp.concatenate([hi, lo], axis=0), rw[b],
                (((1,), (0,)), ((), ())), preferred_element_type=F32,
            )
            tmp[2 + b] = o[:NV, :BS] + (o[:NV, BS:] + o[NV:, :BS])

        sq_row = jnp.sum(
            jnp.where(diagonal(), jnp.sum(sq, axis=1, keepdims=True), 0.0), axis=0, keepdims=True
        )
        for b in range(4):
            for v in range(4):
                aout[pl.ds(4 * b + v, NQ, stride=24), :] = tmp[2 + b, pl.ds(v, NQ, stride=4), :]
            aout[pl.ds(17 + b, NQ, stride=24), :] = agg_v[b // 2, b % 2]
        aout[pl.ds(16, NQ, stride=24), :] = jnp.broadcast_to(sq_row, (NQ, BS))
        for b in range(21, 24):
            aout[pl.ds(b, NQ, stride=24), :] = jnp.zeros((NQ, BS), F32)
        sqs[...] = jnp.broadcast_to(sq_row, (8, BS))

        for i, d in enumerate(Q_ORDER[:-1]):
            q = chip_of(*d)
            start(message(aout, q), message(ain, chip), a_send.at[i], a_recv.at[chip], r, q * 2 + 1)
        for i, d in enumerate(Q_ORDER):
            start(line(sqs, 0), line(sqa, chip), o_send.at[i], o_recv.at[chip], other, chip_of(*d) * 2 + 1)
        cp = residual_to(pair)
        cp.start()
        started.append(cp)

        who = lax.broadcasted_iota(jnp.int32, (NAGG, BS), 0).astype(F32)
        acc = [jnp.zeros((NAGG, BS), F32) for _ in range(4)]
        plane_sq = jnp.zeros((1, BS), F32)
        for d in Q_ORDER[::-1]:
            q = chip_of(*d)
            if d == (0, 0):
                t = message(aout, q)[...]
            else:
                remote(message(aout, q), message(ain, q), a_send.at[0], a_recv.at[q], r, c).wait_recv()
                t = message(ain, q)[...]
            for b in range(4):
                sel = who == t[17 + b:18 + b, :]
                for v in range(4):
                    acc[v] = acc[v] + jnp.where(sel, t[4 * b + v:4 * b + v + 1, :], 0.0)
            plane_sq = plane_sq + t[16:17, :]
        for v in range(4):
            slot(chip)[8 * v:8 * v + 8, :] = acc[v]
        for i in range(NQ - 1):
            q = i + (i + NQ - chip) // NQ
            start(slot(chip), slot(chip), b_send.at[2 * i + 1], b_recv.at[chip], r, q * 2 + 1)
        for i in range(NQ):
            start(slot(chip), slot(chip), b_send.at[2 * i], b_recv.at[chip], r, i * 2)

        for d in Q_ORDER[::-1]:
            q = chip_of(*d)
            remote(line(sqs, 0), line(sqa, q), o_send.at[0], o_recv.at[q], r, c).wait_recv()
            plane_sq = plane_sq + line(sqa, q)[...]
        line(sqb, z)[...] = plane_sq
        for i, d in enumerate((4, 3, 5, 2, 6, 1, 7, 0)):
            start(line(sqb, z), line(sqb, z), q_send.at[2 * i], q_recv.at[z], z_row(d), chip * 2)
            if d > 0:
                start(line(sqb, z), line(sqb, z), q_send.at[2 * i + 1], q_recv.at[z], z_row(d), c)
        for d in range(1, NZ):
            j = (z + d) % NZ
            remote(line(sqb, j), line(sqb, j), q_send.at[0], q_recv.at[j], r, c).wait_recv()
        for d in Q_ORDER[:-1]:
            q = chip_of(*d)
            remote(slot(q), slot(q), b_send.at[0], b_recv.at[q], r, c).wait_recv()
        for cp in started:
            cp.wait_send()

    for cp in sends:
        cp.wait_send()


def finish(cbuf, sqb, resid, coarse_out, resid_out):
    all_sq = jnp.sum(sqb[pl.ds(0, NZ, stride=8), :], axis=0, keepdims=True)
    mean = all_sq * (1.0 / (NR * GR * BS)) + 1e-6
    mean_v = jnp.sum(jnp.where(diagonal(), jnp.broadcast_to(mean, (NV, BS)), 0.0), axis=1, keepdims=True)
    inv = jnp.broadcast_to(1.0 / jnp.sqrt(mean_v), (NV, BS))
    for a in range(NAGG):
        coarse_out[a] = cbuf[pl.ds(a, NV, stride=8), :] * inv
    resid_out[...] = resid[...]


def local(matrix, columns, counts, fine_guess, right_side, aggregate, restrict):
    dma = pltpu.SemaphoreType.DMA
    vmem = pl.BlockSpec(memory_space=pltpu.VMEM)
    parts = pl.pallas_call(
        kernel,
        out_shape=(
            pltpu.VMEM((NC * 16, BS), F32),
            pltpu.VMEM((NZ * 8, BS), F32),
            pltpu.VMEM((2, NV, BS), F32),
        ),
        in_specs=[pl.BlockSpec(memory_space=pltpu.HBM)] * 7,
        out_specs=(vmem,) * 3,
        scratch_shapes=[
            pltpu.VMEM((GR, KB, BS, BS), F32),
            pltpu.VMEM((GR, 2 * BS, KB * BS), BF16),
            pltpu.VMEM((2 * NR, NV, BS), F32),
            pltpu.VMEM((NQ, 2, NV, BS), F32),
            pltpu.VMEM((NQ, 2, NV, BS), F32),
            pltpu.VMEM((NQ, 2, NV, BS), F32),
            pltpu.VMEM((NC, 2, NV, BS), F32),
            pltpu.VMEM((NQ * 24, BS), F32),
            pltpu.VMEM((NQ * 24, BS), F32),
            pltpu.VMEM((2, 2, NV, BS), F32),
            pltpu.VMEM((2, 2, BS, BS), F32),
            pltpu.VMEM((2, 2, 8, BS), F32),
            pltpu.VMEM((4, BS, 2 * BS), BF16),
            pltpu.VMEM((6, NV, BS), F32),
            pltpu.VMEM((8, BS), F32),
            pltpu.VMEM((NQ * 8, BS), F32),
            pltpu.SMEM((KB, GR), jnp.int32),
            pltpu.SMEM((1, GR), jnp.int32),
            pltpu.SMEM((2,), jnp.int32),
            dma((CHUNKS,)), dma((6,)),
            dma((24,)), dma((2 * NR,)),
            dma((NQ,)), dma((NQ,)),
            dma((NQ,)), dma((NC,)),
            dma((4,)), dma((4,)),
            dma((NQ,)), dma((NQ,)),
            dma((NC,)), dma((NQ,)),
            dma((NQ,)), dma((NQ,)),
            dma((NC,)), dma((NZ,)),
            pltpu.SemaphoreType.REGULAR((3,)),
        ],
        compiler_params=pltpu.CompilerParams(collective_id=0, has_side_effects=True, vmem_limit_bytes=60 * 2**20),
    )(matrix, columns.T, counts.T, fine_guess, right_side, aggregate, restrict)
    return pl.pallas_call(
        finish,
        out_shape=(
            jax.ShapeDtypeStruct((NAGG, NV, BS), F32),
            jax.ShapeDtypeStruct((2, NV, BS), F32),
        ),
        in_specs=[vmem] * 3,
        out_specs=(vmem,) * 2,
        compiler_params=pltpu.CompilerParams(vmem_limit_bytes=4 * 2**20),
    )(*parts)


def solution(mesh):
    in_specs = (
        P("row", "col", None, None),
        P("row", "col"),
        P("row", "col"),
        P(("col", "row"), None, None),
        P(("row", "col"), None, None),
        P(("row", "col")),
        P(("row", "col"), None, None),
    )
    out_specs = (P("row", None, None), P(("row", "col"), None, None))
    return jax.shard_map(local, mesh=mesh, in_specs=in_specs, out_specs=out_specs, check_vma=False)
```
